32 devices in a mesh: grp: 2 (over y), subj: 4 (over x, core), vert: 4 (over z).
Axes of the slice: x: 2, y: 2, z: 4, core: 2. Of those that a mesh axis runs over, the one named last changes fastest.
Arguments:
- dosage: bfloat16 [16384, 512], P(('grp', 'subj')), parts along dimension 0, may hold values from 0 to 2
- phenotype: bfloat16 [16384, 20480], P(('grp', 'subj'), 'vert'), parts along dimension 0, may hold values from -12 to 12
- covariates: float32 [16384, 40], P(('grp', 'subj')), parts along dimension 0, may hold values from -7 to 7
Outputs:
- tstat: float32 [1024, 20480], P(('grp', 'subj'), 'vert'), parts along dimension 0
The draws below stay inside these ranges and needn't reach their ends.
There are 2 independent parts, one for each index of `grp`. The reference program is written for one: setup_inputs(seed, part) draws one part's arguments, and reference() takes and returns one part's arrays. A program takes and returns all parts, laid end to end along the dimension named above; each array names one. Nothing has to cross between parts.
All inputs are finite; a program needn't handle non-finite values.
Results may differ from the reference program's by a relative error of at most 0.004.
Values sent between devices are 32-bit elements; how exact they have to be, the bound alone decides.
No kernel may reach another device: no remote copies, remote signals or barrier semaphores. Data moves between devices by JAX's collectives and lax.ppermute only.
A program may use at most 192 MiB of HBM per device.

```python
import jax
import jax.numpy as jnp
from jax import lax

COVS = 40
VERTS = 20480
SNPS = 512
SUBJECTS = 8192


def covariate_table(key):
    base = jax.random.fold_in(key, 101)
    key_vals, key_scale, key_centre = jax.random.split(base, 3)
    scale = jnp.exp(jax.random.uniform(key_scale, (COVS,), jnp.float32, jnp.log(0.5), jnp.log(2.0)))
    centre = jax.random.uniform(key_centre, (COVS,), jnp.float32, -1.0, 1.0)
    raw = jnp.clip(jax.random.normal(key_vals, (SUBJECTS, COVS), jnp.float32), -3.0, 3.0)
    return raw * scale[None, :] + centre[None, :]


def draw_covariates(key, part):
    return covariate_table(key)


def draw_phenotype(key, part):
    table = covariate_table(key)
    key_effect, key_noise = jax.random.split(jax.random.fold_in(key, 202), 2)
    effect = jax.random.normal(key_effect, (COVS, VERTS), jnp.float32) * (0.8 / COVS ** 0.5)
    noise = jax.random.normal(key_noise, (SUBJECTS, VERTS), jnp.float32)
    fitted = jnp.dot(table, effect, precision=lax.Precision.HIGHEST)
    return jnp.clip(fitted + noise, -12.0, 12.0).astype(jnp.bfloat16)


def draw_dosage(key, part):
    table = covariate_table(key)
    key_load, key_base, key_noise = jax.random.split(jax.random.fold_in(key, 303), 3)
    column = jnp.arange(COVS)
    strong = column < max(COVS // 4, 1)
    spread = jnp.where(strong, 0.4, 0.05).astype(jnp.float32)
    loading = jax.random.normal(key_load, (COVS, SNPS), jnp.float32) * spread[:, None]
    offset = jax.random.uniform(key_base, (SNPS,), jnp.float32, -2.5, 1.0)
    noise = jax.random.normal(key_noise, (SUBJECTS, SNPS), jnp.float32)
    logit = offset[None, :] + jnp.dot(table, loading, precision=lax.Precision.HIGHEST) + noise
    return (2.0 * jax.nn.sigmoid(logit)).astype(jnp.bfloat16)


def setup_inputs(seed: int = 0, part: int = 0) -> dict:
    key_list = jax.random.split(jax.random.key(seed), 4)
    part_splits = jax.random.split(jax.random.fold_in(key_list[3], part), 4)
    return {
        "dosage": draw_dosage(jax.random.fold_in(jax.random.fold_in(key_list[3], part), 71), part),
        "phenotype": draw_phenotype(jax.random.fold_in(jax.random.fold_in(key_list[3], part), 71), part),
        "covariates": draw_covariates(jax.random.fold_in(jax.random.fold_in(key_list[3], part), 71), part),
    }


def reference(dosage, phenotype, covariates):
    count = covariates.shape[0]
    design = jnp.concatenate([jnp.ones((count, 1), jnp.float32), covariates], axis=1)
    hi = lax.Precision.HIGHEST
    geno = dosage.astype(jnp.float32)
    pheno = phenotype.astype(jnp.float32)
    gram = jnp.dot(design.T, design, precision=hi)
    factor = jnp.linalg.cholesky(gram)
    geno_coef = jax.scipy.linalg.cho_solve((factor, True), jnp.dot(design.T, geno, precision=hi))
    pheno_coef = jax.scipy.linalg.cho_solve((factor, True), jnp.dot(design.T, pheno, precision=hi))
    geno_res = geno - jnp.dot(design, geno_coef, precision=hi)
    pheno_res = pheno - jnp.dot(design, pheno_coef, precision=hi)
    geno_var = lax.optimization_barrier(jnp.sum(geno_res * geno_res, axis=0))
    pheno_var = lax.optimization_barrier(jnp.sum(pheno_res * pheno_res, axis=0))
    cross = jnp.dot(geno_res.astype(jnp.bfloat16).T.astype(jnp.float32), pheno_res.astype(jnp.bfloat16).astype(jnp.float32), preferred_element_type=jnp.float32)
    dof = jnp.float32(count - covariates.shape[1] - 2)
    return cross * jnp.sqrt(dof) / jnp.sqrt(geno_var[:, None] * pheno_var[None, :] - cross * cross)
```

```python
import functools

import jax
import jax.numpy as jnp
from jax import lax
from jax.experimental import pallas as pl
from jax.experimental.pallas import tpu as pltpu
from jax.sharding import PartitionSpec as P

HI = lax.Precision.HIGHEST
F32 = jnp.float32
BF16 = jnp.bfloat16
LANES = 128
LAST = (((1,), (1,)), ((), ()))


def round_up(value, unit):
    return -(-value // unit) * unit


def split_three(values):
    upper = values.astype(BF16)
    rest = values - upper.astype(F32)
    middle = rest.astype(BF16)
    lower = (rest - middle.astype(F32)).astype(BF16)
    return upper, middle, lower


def prepare_kernel(chips, rows, place_ref, geno_ref, cov_ref, left_ref, give_ref, keep_ref, turned, small):
    chip, core = place_ref[0], place_ref[1]
    covs, subjects = cov_ref.shape
    half = give_ref.shape[0] - chips * rows
    turned[...] = geno_ref[...].T
    for slot in range(chips):
        target = lax.rem(chip + slot + 1, chips) * (2 * rows)
        for side, own in ((0, 1 - core), (1, core)):
            base = (side * chips + slot) * rows
            start = pl.multiple_of(target + own * rows, rows)
            left_ref[base : base + rows, :] = turned[pl.ds(start, rows), :]
    design = jnp.concatenate(
        [jnp.ones((1, subjects), F32), cov_ref[...], jnp.zeros((LANES - covs - 1, subjects), F32)], axis=0
    )
    snps = 2 * chips * rows
    parts = split_three(design)
    for index, part in enumerate(parts):
        left_ref[snps + index * 2 * half : snps + (index + 1) * 2 * half, :] = part[: 2 * half, :]
    geno = left_ref[0:snps, :]
    product = sum(
        lax.dot_general(geno, part, LAST, preferred_element_type=F32) for part in reversed(parts)
    )
    wide = geno.astype(F32)
    square = jnp.sum(wide * wide, axis=1, keepdims=True)
    lane = lax.broadcasted_iota(jnp.int32, (snps, LANES), 1)
    product = jnp.where(lane == covs + 1, square, product)
    give_ref[0 : chips * rows, :] = product[: chips * rows]
    keep_ref[0 : chips * rows, :] = product[chips * rows :]
    small[...] = lax.dot_general(design[: 2 * half], design, LAST, precision=HI, preferred_element_type=F32)
    give_ref[chips * rows :, :] = small[pl.ds(pl.multiple_of((1 - core) * half, half), half), :]
    keep_ref[chips * rows :, :] = small[pl.ds(pl.multiple_of(core * half, half), half), :]


def prepare(place, dosage, cov_rows, chips, rows, half):
    subjects, snps = dosage.shape
    smem = pl.BlockSpec(memory_space=pltpu.SMEM)
    vmem = pl.BlockSpec(memory_space=pltpu.VMEM)
    part = jax.ShapeDtypeStruct((chips * rows + half, LANES), F32)
    return pl.pallas_call(
        functools.partial(prepare_kernel, chips, rows),
        out_shape=(jax.ShapeDtypeStruct((snps + 6 * half, subjects), BF16), part, part),
        in_specs=[smem, vmem, vmem],
        out_specs=(vmem, vmem, vmem),
        scratch_shapes=[pltpu.VMEM((snps, subjects), BF16), pltpu.VMEM((2 * half, LANES), F32)],
        compiler_params=pltpu.CompilerParams(vmem_limit_bytes=40 * 2**20),
        cost_estimate=pl.CostEstimate(
            flops=2 * snps * subjects * 1024, bytes_accessed=4 * snps * subjects, transcendentals=0
        ),
        name="prepare",
    )(place, dosage, cov_rows)


def product_kernel(split, half, row, place_ref, left_ref, pheno_ref, give_ref, keep_ref, small):
    core = place_ref[1]
    pheno = pheno_ref[...]
    result = jnp.dot(left_ref[...], pheno, preferred_element_type=F32)
    give_ref[0:split, :] = result[:split]
    keep_ref[0:split, :] = result[split : 2 * split]
    upper = result[2 * split : 2 * split + 2 * half]
    middle = result[2 * split + 2 * half : 2 * split + 4 * half]
    lower = result[2 * split + 4 * half :]
    wide = pheno.astype(F32)
    square = jnp.sum(wide * wide, axis=0, keepdims=True)
    index = lax.broadcasted_iota(jnp.int32, upper.shape, 0)
    small[...] = jnp.where(index == row, square, (lower + middle) + upper)
    give_ref[split:, :] = small[pl.ds(pl.multiple_of((1 - core) * half, half), half), :]
    keep_ref[split:, :] = small[pl.ds(pl.multiple_of(core * half, half), half), :]


def product(place, left, phenotype, start, width, tile, split, half, row):
    height, subjects = left.shape
    first = start // tile
    part = jax.ShapeDtypeStruct((split + half, width), F32)
    return pl.pallas_call(
        functools.partial(product_kernel, split, half, row),
        grid=(width // tile,),
        out_shape=(part, part),
        in_specs=[
            pl.BlockSpec(memory_space=pltpu.SMEM),
            pl.BlockSpec((height, subjects), lambda j: (0, 0)),
            pl.BlockSpec((subjects, tile), lambda j: (0, first + j)),
        ],
        out_specs=(
            pl.BlockSpec((split + half, tile), lambda j: (0, j)),
            pl.BlockSpec((split + half, tile), lambda j: (0, j)),
        ),
        scratch_shapes=[pltpu.VMEM((2 * half, tile), F32)],
        compiler_params=pltpu.CompilerParams(vmem_limit_bytes=30 * 2**20),
        cost_estimate=pl.CostEstimate(
            flops=2 * height * subjects * width,
            bytes_accessed=2 * subjects * width + 8 * split * width,
            transcendentals=0,
        ),
        name=f"product_{start}",
    )(place, left, phenotype)


def finish_kernel(rank, dof, count, *refs):
    mine_ref, other_ref, white_ref, var_ref, half_ref, rest_ref = refs[:6]
    terms, out_ref = refs[6 : 6 + count], refs[-1]
    mixed = jnp.dot(mine_ref[...], half_ref[...], precision=HI, preferred_element_type=F32)
    mixed = mixed + jnp.dot(other_ref[...], rest_ref[...], precision=HI, preferred_element_type=F32)
    white = mixed[:rank]
    pheno_var = mixed[rank : rank + 1] - jnp.sum(white * white, axis=0, keepdims=True)
    fitted = jnp.dot(white_ref[...], white, precision=HI, preferred_element_type=F32)
    cross = terms[0][...]
    for term in terms[1:]:
        cross = cross + term[...]
    cross = cross - fitted
    out_ref[...] = cross * dof * lax.rsqrt(var_ref[:, 0:1] * pheno_var - cross * cross)


def finish(done, total, start, tile, dof, mine, other, white, geno_var, half_rows, rest_rows, terms):
    rows, width = terms[0].shape
    rank = white.shape[1]
    first = start // tile
    whole = lambda a: pl.BlockSpec(a.shape, lambda j: (0, 0))
    block = lambda a: pl.BlockSpec((a.shape[0], tile), lambda j: (0, j))
    args = [mine, other, white, geno_var, half_rows, rest_rows, *terms]
    specs = [whole(a) for a in args[:4]] + [block(a) for a in args[4:]]
    aliases = {}
    if done is not None:
        aliases = {len(args): 0}
        args.append(done)
        specs.append(pl.BlockSpec(memory_space=pl.ANY))
    return pl.pallas_call(
        functools.partial(finish_kernel, rank, dof, len(terms)),
        grid=(width // tile,),
        out_shape=jax.ShapeDtypeStruct((rows, total), F32),
        in_specs=specs,
        out_specs=pl.BlockSpec((rows, tile), lambda j: (0, first + j)),
        input_output_aliases=aliases,
        compiler_params=pltpu.CompilerParams(vmem_limit_bytes=16 * 2**20),
        cost_estimate=pl.CostEstimate(
            flops=2 * 256 * 256 * width, bytes_accessed=16 * rows * width, transcendentals=rows * width
        ),
        name=f"finish_{start}",
    )(*args)


def chunk_widths(total, unit):
    units = total // unit
    if total % unit or units < 4:
        return [total]
    sizes = [2]
    left = units - 4
    while left > 0:
        sizes.append(min(4, left))
        left -= sizes[-1]
    sizes.append(2)
    return [size * unit for size in sizes]


def per_device(dosage, phenotype, covariates):
    devices = lax.axis_size("subj")
    chips = devices // 2
    subjects, snps = dosage.shape
    verts = phenotype.shape[1]
    covs = covariates.shape[1]
    rank = covs + 1
    rows = snps // devices
    half = round_up(covs + 2, 16) // 2
    split = chips * rows
    far = (chips - 1) * rows
    place_index = lax.axis_index("subj")
    core = lax.rem(place_index, 2)
    place = jnp.stack([place_index // 2, core]).astype(jnp.int32)
    sibling = [(i, i ^ 1) for i in range(devices)]

    def reduce_far(give, keep):
        got = lax.ppermute(give, "subj", sibling)
        near = keep[far:split] + got[far:split]
        own_half = keep[split:] + got[split:]
        terms = [near]
        halves = own_half
        for step in range(1, chips):
            low = (step - 1) * rows
            block = jnp.concatenate([keep[low : low + rows] + got[low : low + rows], own_half], axis=0)
            moves = [(i, (i + 2 * step) % devices) for i in range(devices)]
            came = lax.ppermute(block, "subj", moves)
            terms.append(came[:rows])
            halves = halves + came[rows:]
        rest = lax.ppermute(halves, "subj", sibling)
        return terms, halves, rest

    left, give, keep = prepare(place, dosage, covariates.T, chips, rows, half)
    terms, halves, rest = reduce_far(give, keep)
    own = sum(terms[1:], terms[0])
    low_half = jnp.where(core == 0, halves, rest)
    high_half = jnp.where(core == 0, rest, halves)
    gram = jnp.concatenate([low_half, high_half], axis=0)[:rank, :rank]
    factor = jnp.linalg.cholesky(gram)
    inverse = jax.scipy.linalg.solve_triangular(factor, jnp.eye(rank, dtype=F32), lower=True)
    white = jnp.dot(own[:, :rank], inverse.T, precision=HI)
    geno_var = own[:, rank] - jnp.sum(white * white, axis=1)
    geno_var = jnp.broadcast_to(geno_var[:, None], (rows, LANES))
    mixer = jnp.zeros((rank + 1, 2 * half), F32).at[:rank, :rank].set(inverse).at[rank, rank].set(1.0)
    mine = jnp.where(core == 0, mixer[:, :half], mixer[:, half:])
    other = jnp.where(core == 0, mixer[:, half:], mixer[:, :half])
    dof = float(subjects * devices - covs - 2) ** 0.5

    unit = 256
    out = None
    start = 0
    for width in chunk_widths(verts, unit):
        tile = unit if width % unit == 0 else LANES
        give, keep = product(place, left, phenotype, start, width, tile, split, half, rank)
        terms, halves, rest = reduce_far(give, keep)
        out = finish(out, verts, start, tile, dof, mine, other, white, geno_var, halves, rest, terms)
        start += width
    return out


def solution(mesh):
    in_specs = (P(("grp", "subj"), None), P(("grp", "subj"), "vert"), P(("grp", "subj"), None))
    out_specs = P(("grp", "subj"), "vert")
    return jax.shard_map(
        per_device, mesh=mesh, in_specs=in_specs, out_specs=out_specs, check_vma=False
    )
```

```python
import functools

import jax
import jax.numpy as jnp
from jax import lax
from jax.experimental import pallas as pl
from jax.experimental.pallas import tpu as pltpu
from jax.sharding import PartitionSpec as P


HI = lax.Precision.HIGHEST
F32 = jnp.float32
BF16 = jnp.bfloat16
LANES = 128
TILE = 512
STRIP = 256
SQUARE = 1
OPEN_LIMIT = 20 * 2**20
LIMIT = 12 * 2**20
PIECES = 4
LAST = (((1,), (1,)), ((), ()))


def round_up(value, unit):
    return -(-value // unit) * unit


def split_three(values):
    upper = values.astype(BF16)
    rest = values - upper.astype(F32)
    middle = rest.astype(BF16)
    lower = (rest - middle.astype(F32)).astype(BF16)
    return upper, middle, lower


def block_copies(source, target, sems, first, axis):
    count = PIECES if axis == 0 else max(target.shape[1] // STRIP, 1)
    step = target.shape[axis] // count
    copies = []
    for i in range(count):
        part = (slice(i * step, (i + 1) * step), slice(None))[:: 1 if axis == 0 else -1]
        copies.append(pltpu.make_async_copy(source.at[part], target.at[part], sems.at[first + i]))
    return copies


def column_block(ref, start, width):
    return ref.at[:, start : start + width]


def multiply(left_ref, pheno_ref, copies, outs, small, core, rows, half):
    give_far, give_near, keep_far, keep_near = outs
    width = give_far.shape[1]
    far = give_far.shape[0] - half
    split = far + rows
    step = min(STRIP, width) if copies else min(TILE, width)
    for low in range(0, width, step):
        high = low + step
        if copies:
            copies[low // step].wait()
        pheno = pheno_ref[:, low:high]
        result = jnp.dot(left_ref[...], pheno, preferred_element_type=F32)
        give_far[0:far, low:high] = result[:far]
        give_near[:, low:high] = result[far:split]
        keep_far[0:far, low:high] = result[split : split + far]
        keep_near[:, low:high] = result[split + far : 2 * split]
        upper = result[2 * split : 2 * split + 2 * half]
        middle = result[2 * split + 2 * half : 2 * split + 4 * half]
        lower = result[2 * split + 4 * half :]
        wide = pheno.astype(F32)
        square = jnp.sum(wide * wide, axis=0, keepdims=True)
        place = lax.broadcasted_iota(jnp.int32, upper.shape, 0)
        small[:, low:high] = jnp.where(place == SQUARE, square, (lower + middle) + upper)
    give_far[far:, :] = small[pl.ds(pl.multiple_of((1 - core) * half, half), half), :]
    keep_far[far:, :] = small[pl.ds(pl.multiple_of(core * half, half), half), :]


def part_shapes(chips, rows, half, width):
    far = jax.ShapeDtypeStruct(((chips - 1) * rows + half, width), F32)
    near = jax.ShapeDtypeStruct((rows, width), F32)
    return (far, near, far, near)


def with_design(left_ref, geno, outs, small, core, place, half):
    give_far, _, keep_far, _ = outs
    far = give_far.shape[0] - half
    snps = geno.shape[1]
    size = 2 * half
    design = left_ref[snps:, :]
    product = jnp.dot(design, geno[...], preferred_element_type=F32)
    product = (product[2 * size :] + product[size : 2 * size]) + product[:size]
    wide = geno[...].astype(F32)
    square = jnp.sum(wide * wide, axis=0, keepdims=True)
    row = lax.broadcasted_iota(jnp.int32, (size, snps), 0)
    product = jnp.where(row == SQUARE, square, product)
    product = jnp.concatenate([product, jnp.zeros((LANES - size, snps), F32)], axis=0)
    place[...] = product.T
    gram = lax.dot_general(design, design, LAST, preferred_element_type=F32)
    total = jnp.zeros((size, size), F32)
    for tall, flat in ((2, 0), (0, 2), (1, 1), (1, 0), (0, 1), (0, 0)):
        total = total + gram[tall * size : (tall + 1) * size, flat * size : (flat + 1) * size]
    small[:, 0:LANES] = jnp.concatenate([total, jnp.zeros((size, LANES - size), F32)], axis=1)
    give_far[far:, :] = small[pl.ds(pl.multiple_of((1 - core) * half, half), half), 0:LANES]
    keep_far[far:, :] = small[pl.ds(pl.multiple_of(core * half, half), half), 0:LANES]


def open_kernel(chips, rows, half, widths, place_ref, geno_ref, cov_ref, pheno_ref, *refs):
    left_ref, base, outs = refs[0], refs[1:5], refs[5:9]
    ahead_refs = refs[9:-7]
    geno, turned, design, first, small, table, sems = refs[-7:]
    chip, core = place_ref[0], place_ref[1]
    covs, subjects = cov_ref.shape
    snps = 2 * chips * rows
    cov_copy = pltpu.make_async_copy(cov_ref, design.at[8 : 8 + covs], sems.at[0])
    cov_copy.start()
    geno_copies = block_copies(geno_ref, geno, sems, 1, 0)
    first_copies = block_copies(column_block(pheno_ref, 0, widths[0]), first, sems, 1 + PIECES, 1)
    used = 1 + PIECES + len(first_copies)
    ahead_copies = []
    start = widths[0]
    for index, ahead_ref in enumerate(ahead_refs):
        block = column_block(pheno_ref, start, ahead_ref.shape[1])
        ahead_copies += block_copies(block, ahead_ref, sems, used + index * PIECES, 0)
        start += ahead_ref.shape[1]
    for copy in geno_copies + first_copies + ahead_copies:
        copy.start()
    top = lax.broadcasted_iota(jnp.int32, (8, subjects), 0)
    design[0:8, :] = jnp.where(top == 0, 1.0, 0.0)
    if 2 * half > 8 + covs:
        design[8 + covs :, :] = jnp.zeros((2 * half - 8 - covs, subjects), F32)
    cov_copy.wait()
    for index, part in enumerate(split_three(design[...])):
        left_ref[snps + index * 2 * half : snps + (index + 1) * 2 * half, :] = part
    step = subjects // PIECES
    for index, copy in enumerate(geno_copies):
        copy.wait()
        turned[:, index * step : (index + 1) * step] = geno[index * step : (index + 1) * step, :].T
    with_design(left_ref, geno, base, small, core, table, half)
    for slot in range(chips):
        target = lax.rem(chip + slot + 1, chips) * (2 * rows)
        for side, own in ((0, 1 - core), (1, core)):
            low = (side * chips + slot) * rows
            start = pl.multiple_of(target + own * rows, rows)
            left_ref[low : low + rows, :] = turned[pl.ds(start, rows), :]
            if slot < chips - 1:
                base[2 * side][slot * rows : (slot + 1) * rows, :] = table[pl.ds(start, rows), :]
            else:
                base[2 * side + 1][...] = table[pl.ds(start, rows), :]
    multiply(left_ref, first, first_copies, outs, small, core, rows, half)
    for copy in ahead_copies:
        copy.wait()


def cost(flops, moved):
    return pl.CostEstimate(flops=flops, bytes_accessed=moved, transcendentals=0)


SMEM = pl.BlockSpec(memory_space=pltpu.SMEM)
VMEM = pl.BlockSpec(memory_space=pltpu.VMEM)
HBM = pl.BlockSpec(memory_space=pltpu.HBM)


def open_up(place, dosage, cov_rows, phenotype, chips, rows, half, widths):
    width = widths[0]
    subjects, snps = dosage.shape
    height = snps + 6 * half
    left = jax.ShapeDtypeStruct((height, subjects), BF16)
    ahead = [jax.ShapeDtypeStruct((subjects, later), BF16) for later in widths[1:]]
    parts = part_shapes(chips, rows, half, LANES) + part_shapes(chips, rows, half, width)
    return pl.pallas_call(
        functools.partial(open_kernel, chips, rows, half, widths),
        out_shape=(left, *parts, *ahead),
        in_specs=[SMEM, HBM, HBM, HBM],
        out_specs=(VMEM,) * (9 + len(ahead)),
        scratch_shapes=[
            pltpu.VMEM((subjects, snps), BF16),
            pltpu.VMEM((snps, subjects), BF16),
            pltpu.VMEM((2 * half, subjects), F32),
            pltpu.VMEM((subjects, width), BF16),
            pltpu.VMEM((2 * half, max(width, LANES)), F32),
            pltpu.VMEM((snps, LANES), F32),
            pltpu.SemaphoreType.DMA((1 + len(widths) * PIECES + max(width // STRIP, 1),)),
        ],
        compiler_params=pltpu.CompilerParams(vmem_limit_bytes=OPEN_LIMIT),
        cost_estimate=cost(2 * height * subjects * width, 4 * snps * subjects),
        name="open",
    )(place, dosage, cov_rows, phenotype)


def product_kernel(rows, half, place_ref, left_ref, pheno_ref, *refs):
    multiply(left_ref, pheno_ref, [], refs[:4], refs[4], place_ref[1], rows, half)


def product(place, left, phenotype, chips, rows, half):
    height, subjects = left.shape
    width = phenotype.shape[1]
    return pl.pallas_call(
        functools.partial(product_kernel, rows, half),
        out_shape=part_shapes(chips, rows, half, width),
        in_specs=[SMEM, VMEM, VMEM],
        out_specs=(VMEM,) * 4,
        scratch_shapes=[pltpu.VMEM((2 * half, width), F32)],
        compiler_params=pltpu.CompilerParams(vmem_limit_bytes=LIMIT),
        cost_estimate=cost(2 * height * subjects * width, 2 * subjects * width),
    )(place, left, phenotype)


def solve_kernel(live, half, count, *refs):
    place_ref, half_ref, rest_ref = refs[:3]
    terms, (inverse_ref, white_ref, var_ref, work) = refs[3 : 3 + count], refs[3 + count :]
    core = place_ref[1]
    size = 2 * half
    work[pl.ds(pl.multiple_of(core * half, half), half), :] = half_ref[...]
    work[pl.ds(pl.multiple_of((1 - core) * half, half), half), :] = rest_ref[...]
    row = lax.broadcasted_iota(jnp.int32, (size, LANES), 0)
    lane = lax.broadcasted_iota(jnp.int32, (size, LANES), 1)
    left = jnp.where(lane < size, work[...], 0.0)
    right = jnp.where(lane == row, 1.0, 0.0)
    scaled = jnp.zeros((size, LANES), F32)
    for step in live:
        pivot = jnp.broadcast_to(left[:, step : step + 1], (size, LANES))
        top = jnp.broadcast_to(pivot[step : step + 1], (size, LANES))
        ratio = jnp.where(row > step, pivot / top, 0.0)
        root = lax.rsqrt(top)
        root = root * (1.5 - 0.5 * top * root * root)
        scaled = jnp.where(row == step, right * root, scaled)
        left = left - ratio * left[step : step + 1]
        right = right - ratio * right[step : step + 1]
    inverse_ref[...] = scaled
    own = terms[0][...]
    for term in terms[1:]:
        own = own + term[...]
    wide = jnp.concatenate([scaled, jnp.zeros((LANES - size, LANES), F32)], axis=0)
    white = lax.dot_general(own, wide, LAST, precision=HI, preferred_element_type=F32)
    white_ref[...] = white
    var_ref[...] = jnp.broadcast_to(
        own[:, SQUARE : SQUARE + 1] - jnp.sum(white * white, axis=1, keepdims=True), var_ref.shape
    )


def solve(place, half_rows, rest_rows, terms, live):
    half = half_rows.shape[0]
    wide = jax.ShapeDtypeStruct(terms[0].shape, F32)
    return pl.pallas_call(
        functools.partial(solve_kernel, live, half, len(terms)),
        out_shape=(jax.ShapeDtypeStruct((2 * half, LANES), F32), wide, wide),
        in_specs=[SMEM] + [VMEM] * (2 + len(terms)),
        out_specs=(VMEM,) * 3,
        scratch_shapes=[pltpu.VMEM((2 * half, LANES), F32)],
        compiler_params=pltpu.CompilerParams(vmem_limit_bytes=LIMIT),
        cost_estimate=cost(5 * 10**9, 2**16),
        name="solve",
    )(place, half_rows, rest_rows, *terms)


def finish_kernel(dof, count, *refs):
    place_ref, inverse_ref, white_ref, var_ref, half_ref, rest_ref = refs[:6]
    terms, out_ref, small = refs[6 : 6 + count], refs[-2], refs[-1]
    half = half_ref.shape[0]
    rows, tile = out_ref.shape
    core = place_ref[1]
    low = pl.multiple_of(pl.program_id(0) * tile, tile)
    small[pl.ds(pl.multiple_of(core * half, half), half), :] = half_ref[:, pl.ds(low, tile)]
    small[pl.ds(pl.multiple_of((1 - core) * half, half), half), :] = rest_ref[:, pl.ds(low, tile)]
    white = jnp.dot(inverse_ref[:, : 2 * half], small[...], precision=HI, preferred_element_type=F32)
    pheno_var = small[SQUARE : SQUARE + 1, :] - jnp.sum(white * white, axis=0, keepdims=True)
    fitted = jnp.dot(white_ref[:, : 2 * half], white, precision=HI, preferred_element_type=F32)
    cross = terms[0][0:rows, pl.ds(low, tile)]
    for term in terms[1:]:
        cross = cross + term[0:rows, pl.ds(low, tile)]
    cross = cross - fitted
    out_ref[...] = cross * dof * lax.rsqrt(var_ref[:, 0:1] * pheno_var - cross * cross)


def finish(done, total, place, start, dof, inverse, white, geno_var, half_rows, rest_rows, terms):
    rows, width = terms[0].shape
    tile = min(STRIP, width)
    first = start // tile
    args = [place, inverse, white, geno_var, half_rows, rest_rows, *terms]
    specs = [SMEM] + [VMEM] * (len(args) - 1)
    aliases = {}
    if done is not None:
        aliases = {len(args): 0}
        args.append(done)
        specs.append(HBM)
    return pl.pallas_call(
        functools.partial(finish_kernel, dof, len(terms)),
        grid=(width // tile,),
        out_shape=jax.ShapeDtypeStruct((rows, total), F32),
        in_specs=specs,
        out_specs=pl.BlockSpec((rows, tile), lambda j: (0, first + j)),
        scratch_shapes=[pltpu.VMEM((2 * half_rows.shape[0], tile), F32)],
        input_output_aliases=aliases,
        compiler_params=pltpu.CompilerParams(vmem_limit_bytes=LIMIT),
        cost_estimate=pl.CostEstimate(
            flops=2 * 256 * 256 * width, bytes_accessed=16 * rows * width, transcendentals=rows * width
        ),
    )(*args)


def chunk_widths(total):
    units = total // TILE
    if total % TILE or units < 3:
        return [total]
    sizes = [1]
    left = units - 2
    while left > 0:
        sizes.append(min(2, left))
        left -= sizes[-1]
    sizes.append(1)
    return [size * TILE for size in sizes]


def associate(dosage, phenotype, covariates):
    devices = lax.axis_size("subj")
    chips = devices // 2
    subjects, snps = dosage.shape
    verts = phenotype.shape[1]
    covs = covariates.shape[1]
    rows = snps // devices
    half = round_up(8 + covs, 16) // 2
    live = [0] + list(range(8, 8 + covs))
    far = (chips - 1) * rows
    place_index = lax.axis_index("subj")
    place = jnp.stack([place_index // 2, lax.rem(place_index, 2)]).astype(jnp.int32)
    sibling = [(i, i ^ 1) for i in range(devices)]

    def near_sums(parts):
        give_far, give_near, keep_far, keep_near = parts
        got_far = lax.ppermute(give_far, "subj", sibling)
        got_near = lax.ppermute(give_near, "subj", sibling)
        summed = keep_far + got_far
        if chips == 2:
            return [keep_near, got_near], [summed]
        own_half = summed[far:]
        blocks = [jnp.concatenate([summed[low : low + rows], own_half], axis=0) for low in range(0, far, rows)]
        return [keep_near, got_near], blocks

    def far_terms(blocks):
        came = []
        for step, block in enumerate(blocks, 1):
            moves = [(i, (i + 2 * step) % devices) for i in range(devices)]
            came.append(lax.ppermute(block, "subj", moves))
        return came

    def gather_half(blocks, came):
        halves = blocks[0][rows:]
        for block in came:
            halves = halves + block[rows:]
        rest = lax.ppermute(halves, "subj", sibling)
        return halves, rest

    widths = chunk_widths(verts)
    left, *parts = open_up(
        place, dosage, covariates.T, phenotype, chips, rows, half, widths
    )
    ahead = parts[8:]
    sums = [near_sums(parts[4:8])]
    came = [far_terms(sums[0][1])]
    terms, blocks = near_sums(parts[:4])
    base_came = far_terms(blocks)
    halves, rest = gather_half(blocks, base_came)
    inverse, white, geno_var = solve(
        place, halves, rest, terms + [block[:rows] for block in base_came], live
    )
    dof = float(subjects * devices - covs - 2) ** 0.5

    start = widths[0]
    for index in range(1, len(widths)):
        parts = product(place, left, ahead[index - 1], chips, rows, half)
        start += widths[index]
        sums.append(near_sums(parts))
        came.append(far_terms(sums[-1][1]))
    out = None
    start = 0
    for index, width in enumerate(widths):
        terms, blocks = sums[index]
        halves, rest = gather_half(blocks, came[index])
        out = finish(
            out, verts, place, start, dof, inverse, white, geno_var, halves, rest, terms + came[index]
        )
        start += width
    return out


def solution(mesh):
    in_specs = (P(("grp", "subj"), None), P(("grp", "subj"), "vert"), P(("grp", "subj"), None))
    out_specs = P(("grp", "subj"), "vert")
    return jax.shard_map(associate, mesh=mesh, in_specs=in_specs, out_specs=out_specs, check_vma=False)
```

```python
import functools

import jax
import jax.numpy as jnp
from jax import lax
from jax.experimental import pallas as pl
from jax.experimental.pallas import tpu as pltpu
from jax.sharding import PartitionSpec as P


HI = lax.Precision.HIGHEST
F32 = jnp.float32
BF16 = jnp.bfloat16
LANES = 128
TILE = 512
STRIP = 256
SQUARE = 1
OPEN_LIMIT = 20 * 2**20
LIMIT = 12 * 2**20
PIECES = 4
GROUPS = 4
LAST = (((1,), (1,)), ((), ()))


def round_up(value, unit):
    return -(-value // unit) * unit


def split_three(values):
    upper = values.astype(BF16)
    rest = values - upper.astype(F32)
    middle = rest.astype(BF16)
    lower = (rest - middle.astype(F32)).astype(BF16)
    return upper, middle, lower


def block_copies(source, target, sems, first, axis):
    count = PIECES if axis == 0 else max(target.shape[1] // STRIP, 1)
    step = target.shape[axis] // count
    copies = []
    for i in range(count):
        part = (slice(i * step, (i + 1) * step), slice(None))[:: 1 if axis == 0 else -1]
        copies.append(pltpu.make_async_copy(source.at[part], target.at[part], sems.at[first + i]))
    return copies


def column_block(ref, start, width):
    return ref.at[:, start : start + width]


def multiply(left_ref, pheno_ref, copies, outs, small, core, rows, half):
    give_far, give_near, keep_far, keep_near = outs
    width = give_far.shape[1]
    far = give_far.shape[0] - half
    split = far + rows
    step = min(STRIP, width) if copies else min(TILE, width)
    for low in range(0, width, step):
        high = low + step
        if copies:
            copies[low // step].wait()
        pheno = pheno_ref[:, low:high]
        result = jnp.dot(left_ref[...], pheno, preferred_element_type=F32)
        give_far[0:far, low:high] = result[:far]
        give_near[:, low:high] = result[far:split]
        keep_far[0:far, low:high] = result[split : split + far]
        keep_near[:, low:high] = result[split + far : 2 * split]
        upper = result[2 * split : 2 * split + 2 * half]
        middle = result[2 * split + 2 * half : 2 * split + 4 * half]
        lower = result[2 * split + 4 * half :]
        wide = pheno.astype(F32)
        square = jnp.sum(wide * wide, axis=0, keepdims=True)
        place = lax.broadcasted_iota(jnp.int32, upper.shape, 0)
        small[:, low:high] = jnp.where(place == SQUARE, square, (lower + middle) + upper)
    give_far[far:, :] = small[pl.ds(pl.multiple_of((1 - core) * half, half), half), :]
    keep_far[far:, :] = small[pl.ds(pl.multiple_of(core * half, half), half), :]


def part_shapes(chips, rows, half, width):
    far = jax.ShapeDtypeStruct(((chips - 1) * rows + half, width), F32)
    near = jax.ShapeDtypeStruct((rows, width), F32)
    return (far, near, far, near)


def design_kernel(chips, rows, half, place_ref, left_ref, geno_ref, *refs):
    outs, (small, table) = refs[:4], refs[4:]
    give_far, _, keep_far, _ = outs
    chip, core = place_ref[0], place_ref[1]
    far = give_far.shape[0] - half
    snps = geno_ref.shape[1]
    size = 2 * half
    design = left_ref[snps:, :]
    product = jnp.dot(design, geno_ref[...], preferred_element_type=F32)
    product = (product[2 * size :] + product[size : 2 * size]) + product[:size]
    wide = geno_ref[...].astype(F32)
    square = jnp.sum(wide * wide, axis=0, keepdims=True)
    row = lax.broadcasted_iota(jnp.int32, (size, snps), 0)
    product = jnp.where(row == SQUARE, square, product)
    product = jnp.concatenate([product, jnp.zeros((LANES - size, snps), F32)], axis=0)
    table[...] = product.T
    for slot in range(chips):
        target = lax.rem(chip + slot + 1, chips) * (2 * rows)
        for side, own in ((0, 1 - core), (1, core)):
            start = pl.multiple_of(target + own * rows, rows)
            if slot < chips - 1:
                outs[2 * side][slot * rows : (slot + 1) * rows, :] = table[pl.ds(start, rows), :]
            else:
                outs[2 * side + 1][...] = table[pl.ds(start, rows), :]
    gram = lax.dot_general(design, design, LAST, preferred_element_type=F32)
    total = jnp.zeros((size, size), F32)
    for tall, flat in ((2, 0), (0, 2), (1, 1), (1, 0), (0, 1), (0, 0)):
        total = total + gram[tall * size : (tall + 1) * size, flat * size : (flat + 1) * size]
    small[...] = jnp.concatenate([total, jnp.zeros((size, LANES - size), F32)], axis=1)
    give_far[far:, :] = small[pl.ds(pl.multiple_of((1 - core) * half, half), half), :]
    keep_far[far:, :] = small[pl.ds(pl.multiple_of(core * half, half), half), :]


def with_design(place, left, geno, chips, rows, half):
    subjects, snps = geno.shape
    return pl.pallas_call(
        functools.partial(design_kernel, chips, rows, half),
        out_shape=part_shapes(chips, rows, half, LANES),
        in_specs=[SMEM, VMEM, VMEM],
        out_specs=(VMEM,) * 4,
        scratch_shapes=[pltpu.VMEM((2 * half, LANES), F32), pltpu.VMEM((snps, LANES), F32)],
        compiler_params=pltpu.CompilerParams(vmem_limit_bytes=LIMIT),
        cost_estimate=cost(2 * 6 * half * subjects * snps, 2 * subjects * snps),
        name="with_design",
    )(place, left, geno)


def open_kernel(chips, rows, half, widths, place_ref, geno_ref, cov_ref, pheno_ref, *refs):
    left_ref, geno, outs = refs[0], refs[1], refs[2:6]
    ahead_refs = refs[6:-5]
    turned, design, first, small, sems = refs[-5:]
    chip, core = place_ref[0], place_ref[1]
    covs, subjects = cov_ref.shape
    snps = 2 * chips * rows
    cov_copy = pltpu.make_async_copy(cov_ref, design.at[8 : 8 + covs], sems.at[0])
    cov_copy.start()
    geno_copies = block_copies(geno_ref, geno, sems, 1, 0)
    first_copies = block_copies(column_block(pheno_ref, 0, widths[0]), first, sems, 1 + PIECES, 1)
    used = 1 + PIECES + len(first_copies)
    ahead_copies = []
    start = widths[0]
    for index, ahead_ref in enumerate(ahead_refs):
        block = column_block(pheno_ref, start, ahead_ref.shape[1])
        ahead_copies += block_copies(block, ahead_ref, sems, used + index * PIECES, 0)
        start += ahead_ref.shape[1]
    for copy in geno_copies + first_copies:
        copy.start()
    top = lax.broadcasted_iota(jnp.int32, (8, subjects), 0)
    design[0:8, :] = jnp.where(top == 0, 1.0, 0.0)
    if 2 * half > 8 + covs:
        design[8 + covs :, :] = jnp.zeros((2 * half - 8 - covs, subjects), F32)
    cov_copy.wait()
    for index, part in enumerate(split_three(design[...])):
        left_ref[snps + index * 2 * half : snps + (index + 1) * 2 * half, :] = part
    step = subjects // GROUPS
    for index in range(GROUPS):
        for copy in geno_copies[index * PIECES // GROUPS : (index + 1) * PIECES // GROUPS]:
            copy.wait()
        turned[:, index * step : (index + 1) * step] = geno[index * step : (index + 1) * step, :].T
    for copy in ahead_copies:
        copy.start()
    for slot in range(chips):
        target = lax.rem(chip + slot + 1, chips) * (2 * rows)
        for side, own in ((0, 1 - core), (1, core)):
            low = (side * chips + slot) * rows
            start = pl.multiple_of(target + own * rows, rows)
            left_ref[low : low + rows, :] = turned[pl.ds(start, rows), :]
    multiply(left_ref, first, first_copies, outs, small, core, rows, half)
    for copy in ahead_copies:
        copy.wait()


def cost(flops, moved):
    return pl.CostEstimate(flops=flops, bytes_accessed=moved, transcendentals=0)


def in_hbm(array):
    return pltpu.with_memory_space_constraint(array, pltpu.HBM)


SMEM = pl.BlockSpec(memory_space=pltpu.SMEM)
VMEM = pl.BlockSpec(memory_space=pltpu.VMEM)
HBM = pl.BlockSpec(memory_space=pltpu.HBM)


def open_up(place, dosage, cov_rows, phenotype, chips, rows, half, widths):
    width = widths[0]
    subjects, snps = dosage.shape
    height = snps + 6 * half
    left = jax.ShapeDtypeStruct((height, subjects), BF16)
    ahead = [jax.ShapeDtypeStruct((subjects, later), BF16) for later in widths[1:2]]
    geno = jax.ShapeDtypeStruct((subjects, snps), BF16)
    parts = part_shapes(chips, rows, half, width)
    return pl.pallas_call(
        functools.partial(open_kernel, chips, rows, half, widths),
        out_shape=(left, geno, *parts, *ahead),
        in_specs=[SMEM, HBM, HBM, HBM],
        out_specs=(VMEM,) * (6 + len(ahead)),
        scratch_shapes=[
            pltpu.VMEM((snps, subjects), BF16),
            pltpu.VMEM((2 * half, subjects), F32),
            pltpu.VMEM((subjects, width), BF16),
            pltpu.VMEM((2 * half, width), F32),
            pltpu.SemaphoreType.DMA((1 + 2 * PIECES + max(width // STRIP, 1),)),
        ],
        compiler_params=pltpu.CompilerParams(vmem_limit_bytes=OPEN_LIMIT),
        cost_estimate=cost(2 * height * subjects * width, 4 * snps * subjects),
        name="open",
    )(place, in_hbm(dosage), in_hbm(cov_rows), in_hbm(phenotype))


def product_kernel(rows, half, start, place_ref, left_ref, here_ref, pheno_ref, *refs):
    outs, later, (small, sems) = refs[:4], refs[4:-2], refs[-2:]
    core = place_ref[1]
    copies = []
    for target in later:
        copies += block_copies(column_block(pheno_ref, start, target.shape[1]), target, sems, 0, 0)
    for copy in copies:
        copy.start()

    @pl.when(core >= 0)
    def _():
        multiply(left_ref, here_ref, [], outs, small, core, rows, half)

    for copy in copies:
        copy.wait()


def product(place, left, here, phenotype, start, later, chips, rows, half):
    height, subjects = left.shape
    width = here.shape[1]
    ahead = [jax.ShapeDtypeStruct((subjects, size), BF16) for size in later]
    return pl.pallas_call(
        functools.partial(product_kernel, rows, half, start + width),
        out_shape=(*part_shapes(chips, rows, half, width), *ahead),
        in_specs=[SMEM, VMEM, VMEM, HBM],
        out_specs=(VMEM,) * (4 + len(ahead)),
        scratch_shapes=[pltpu.VMEM((2 * half, width), F32), pltpu.SemaphoreType.DMA((PIECES,))],
        compiler_params=pltpu.CompilerParams(vmem_limit_bytes=LIMIT),
        cost_estimate=cost(2 * height * subjects * width, 2 * subjects * width),
    )(place, left, here, in_hbm(phenotype))


def solve_kernel(live, half, count, *refs):
    place_ref, half_ref, rest_ref = refs[:3]
    terms, (inverse_ref, white_ref, var_ref, work) = refs[3 : 3 + count], refs[3 + count :]
    core = place_ref[1]
    size = 2 * half
    work[pl.ds(pl.multiple_of(core * half, half), half), :] = half_ref[...]
    work[pl.ds(pl.multiple_of((1 - core) * half, half), half), :] = rest_ref[...]
    row = lax.broadcasted_iota(jnp.int32, (size, LANES), 0)
    lane = lax.broadcasted_iota(jnp.int32, (size, LANES), 1)
    left = jnp.where(lane < size, work[...], 0.0)
    right = jnp.where(lane == row, 1.0, 0.0)
    scaled = jnp.zeros((size, LANES), F32)
    for step in live:
        pivot = jnp.broadcast_to(left[:, step : step + 1], (size, LANES))
        top = jnp.broadcast_to(pivot[step : step + 1], (size, LANES))
        ratio = jnp.where(row > step, pivot / top, 0.0)
        root = lax.rsqrt(top)
        root = root * (1.5 - 0.5 * top * root * root)
        scaled = jnp.where(row == step, right * root, scaled)
        left = left - ratio * left[step : step + 1]
        right = right - ratio * right[step : step + 1]
    inverse_ref[...] = scaled
    own = terms[0][...]
    for term in terms[1:]:
        own = own + term[...]
    wide = jnp.concatenate([scaled, jnp.zeros((LANES - size, LANES), F32)], axis=0)
    white = lax.dot_general(own, wide, LAST, precision=HI, preferred_element_type=F32)
    white_ref[...] = white
    var_ref[...] = jnp.broadcast_to(
        own[:, SQUARE : SQUARE + 1] - jnp.sum(white * white, axis=1, keepdims=True), var_ref.shape
    )


def solve(place, half_rows, rest_rows, terms, live):
    half = half_rows.shape[0]
    wide = jax.ShapeDtypeStruct(terms[0].shape, F32)
    return pl.pallas_call(
        functools.partial(solve_kernel, live, half, len(terms)),
        out_shape=(jax.ShapeDtypeStruct((2 * half, LANES), F32), wide, wide),
        in_specs=[SMEM] + [VMEM] * (2 + len(terms)),
        out_specs=(VMEM,) * 3,
        scratch_shapes=[pltpu.VMEM((2 * half, LANES), F32)],
        compiler_params=pltpu.CompilerParams(vmem_limit_bytes=LIMIT),
        cost_estimate=cost(5 * 10**9, 2**16),
        name="solve",
    )(place, half_rows, rest_rows, *terms)


def finish_kernel(dof, count, *refs):
    place_ref, inverse_ref, white_ref, var_ref, half_ref, rest_ref = refs[:6]
    terms, out_ref, small = refs[6 : 6 + count], refs[-2], refs[-1]
    half = half_ref.shape[0]
    rows, tile = out_ref.shape
    core = place_ref[1]
    low = pl.multiple_of(pl.program_id(0) * tile, tile)
    small[pl.ds(pl.multiple_of(core * half, half), half), :] = half_ref[:, pl.ds(low, tile)]
    small[pl.ds(pl.multiple_of((1 - core) * half, half), half), :] = rest_ref[:, pl.ds(low, tile)]
    white = jnp.dot(inverse_ref[:, : 2 * half], small[...], precision=HI, preferred_element_type=F32)
    pheno_var = small[SQUARE : SQUARE + 1, :] - jnp.sum(white * white, axis=0, keepdims=True)
    fitted = jnp.dot(white_ref[:, : 2 * half], white, precision=HI, preferred_element_type=F32)
    cross = terms[0][0:rows, pl.ds(low, tile)]
    for term in terms[1:]:
        cross = cross + term[0:rows, pl.ds(low, tile)]
    cross = cross - fitted
    out_ref[...] = cross * dof * lax.rsqrt(var_ref[:, 0:1] * pheno_var - cross * cross)


def finish(done, total, place, start, dof, inverse, white, geno_var, half_rows, rest_rows, terms):
    rows, width = terms[0].shape
    tile = min(TILE, width)
    first = start // tile
    args = [place, inverse, white, geno_var, half_rows, rest_rows, *terms]
    specs = [SMEM] + [VMEM] * (len(args) - 1)
    aliases = {}
    if done is not None:
        aliases = {len(args): 0}
        args.append(done)
        specs.append(HBM)
    return pl.pallas_call(
        functools.partial(finish_kernel, dof, len(terms)),
        grid=(width // tile,),
        out_shape=jax.ShapeDtypeStruct((rows, total), F32),
        in_specs=specs,
        out_specs=pl.BlockSpec((rows, tile), lambda j: (0, first + j)),
        scratch_shapes=[pltpu.VMEM((2 * half_rows.shape[0], tile), F32)],
        input_output_aliases=aliases,
        compiler_params=pltpu.CompilerParams(vmem_limit_bytes=LIMIT),
        cost_estimate=pl.CostEstimate(
            flops=2 * 256 * 256 * width, bytes_accessed=16 * rows * width, transcendentals=rows * width
        ),
    )(*args)


def fit_kernel(count, *refs):
    place_ref, inverse_ref, white_ref, half_ref, rest_ref = refs[:5]
    terms, (cross_ref, var_ref, small) = refs[5 : 5 + count], refs[5 + count :]
    half = half_ref.shape[0]
    core = place_ref[1]
    small[pl.ds(pl.multiple_of(core * half, half), half), :] = half_ref[...]
    small[pl.ds(pl.multiple_of((1 - core) * half, half), half), :] = rest_ref[...]
    white = jnp.dot(inverse_ref[:, : 2 * half], small[...], precision=HI, preferred_element_type=F32)
    pheno_var = small[SQUARE : SQUARE + 1, :] - jnp.sum(white * white, axis=0, keepdims=True)
    var_ref[...] = jnp.broadcast_to(pheno_var, var_ref.shape)
    fitted = jnp.dot(white_ref[:, : 2 * half], white, precision=HI, preferred_element_type=F32)
    cross = terms[0][...]
    for term in terms[1:]:
        cross = cross + term[...]
    cross_ref[...] = cross - fitted


def fit(place, inverse, white, half_rows, rest_rows, terms):
    rows, width = terms[0].shape
    args = [place, inverse, white, half_rows, rest_rows, *terms]
    return pl.pallas_call(
        functools.partial(fit_kernel, len(terms)),
        out_shape=(jax.ShapeDtypeStruct((rows, width), F32), jax.ShapeDtypeStruct((8, width), F32)),
        in_specs=[SMEM] + [VMEM] * (len(args) - 1),
        out_specs=(VMEM, VMEM),
        scratch_shapes=[pltpu.VMEM((2 * half_rows.shape[0], width), F32)],
        compiler_params=pltpu.CompilerParams(vmem_limit_bytes=LIMIT),
        cost_estimate=cost(2 * 256 * 256 * width, 16 * rows * width),
        name="fit",
    )(*args)


def close_kernel(dof, count, *refs):
    geno_var_ref, pheno_var_ref = refs[:2]
    terms, out_ref = refs[2 : 2 + count], refs[-1]
    tile = out_ref.shape[1]
    low = pl.multiple_of(pl.program_id(0) * tile, tile)
    cross = terms[0][:, pl.ds(low, tile)]
    for term in terms[1:]:
        cross = cross + term[:, pl.ds(low, tile)]
    pheno_var = pheno_var_ref[0:1, pl.ds(low, tile)]
    out_ref[...] = cross * dof * lax.rsqrt(geno_var_ref[:, 0:1] * pheno_var - cross * cross)


def close(done, total, start, dof, geno_var, pheno_var, terms):
    rows, width = terms[0].shape
    tile = min(STRIP, width)
    first = start // tile
    args = [geno_var, pheno_var, *terms]
    specs = [VMEM] * len(args)
    aliases = {}
    if done is not None:
        aliases = {len(args): 0}
        args.append(done)
        specs.append(HBM)
    return pl.pallas_call(
        functools.partial(close_kernel, dof, len(terms)),
        grid=(width // tile,),
        out_shape=jax.ShapeDtypeStruct((rows, total), F32),
        in_specs=specs,
        out_specs=pl.BlockSpec((rows, tile), lambda j: (0, first + j)),
        input_output_aliases=aliases,
        compiler_params=pltpu.CompilerParams(vmem_limit_bytes=LIMIT),
        cost_estimate=cost(8 * rows * width, 12 * rows * width),
        name="close",
    )(*args)


def chunk_widths(total):
    units = total // TILE
    if total % TILE or units < 2:
        return [total]
    wide, odd = divmod(max(units - 4, 0), 2)
    sizes = [1] * min(units - units // 2, 2) + [2] * wide + [1] * odd + [1] * min(units // 2, 2)
    return [size * TILE for size in sizes]


def associate(dosage, phenotype, covariates):
    devices = lax.axis_size("subj")
    chips = devices // 2
    subjects, snps = dosage.shape
    verts = phenotype.shape[1]
    covs = covariates.shape[1]
    rows = snps // devices
    half = round_up(8 + covs, 16) // 2
    live = [0] + list(range(8, 8 + covs))
    far = (chips - 1) * rows
    place_index = lax.axis_index("subj")
    place = jnp.stack([place_index // 2, lax.rem(place_index, 2)]).astype(jnp.int32)
    sibling = [(i, i ^ 1) for i in range(devices)]

    def near_sums(parts, apart=False):
        give_far, give_near, keep_far, keep_near = parts
        got_far = lax.ppermute(give_far, "subj", sibling)
        got_near = lax.ppermute(give_near, "subj", sibling)
        terms = [keep_near, got_near]
        if apart:
            blocks = [keep_far[low : low + rows] + got_far[low : low + rows] for low in range(0, far, rows)]
            return terms, blocks, keep_far[far:] + got_far[far:]
        summed = keep_far + got_far
        if chips == 2:
            return terms, [summed], summed[rows:]
        own_half = summed[far:]
        blocks = [jnp.concatenate([summed[low : low + rows], own_half], axis=0) for low in range(0, far, rows)]
        return terms, blocks, own_half

    def far_terms(blocks):
        came = []
        for step, block in enumerate(blocks, 1):
            moves = [(i, (i + 2 * step) % devices) for i in range(devices)]
            came.append(lax.ppermute(block, "subj", moves))
        return came

    def gather_half(halves, came):
        for block in came:
            halves = halves + block
        rest = lax.ppermute(halves, "subj", sibling)
        return halves, rest

    widths = chunk_widths(verts)
    last = len(widths)
    left, geno, *parts = open_up(
        place, dosage, covariates.T, phenotype, chips, rows, half, widths
    )
    ahead = parts[4:]
    sums = [near_sums(parts[:4])]
    came = [far_terms(sums[0][1])]
    parts = with_design(place, left, geno, chips, rows, half)
    terms, blocks, own_half = near_sums(parts)
    base_came = far_terms(blocks)
    halves, rest = gather_half(own_half, [block[rows:] for block in base_came])
    inverse, white, geno_var = solve(
        place, halves, rest, terms + [block[:rows] for block in base_came], live
    )
    dof = float(subjects * devices - covs - 2) ** 0.5

    start = widths[0]
    for index in range(1, last):
        tag = index + 1
        parts = product(
            place, left, ahead[0], phenotype, start, widths[index + 1 : index + 2], chips, rows, half
        )
        ahead = parts[4:]
        start += widths[index]
        sums.append(near_sums(parts[:4], apart=tag == last))
        if tag == last:
            last_half = far_terms([sums[-1][2]] * (chips - 1))
        came.append(far_terms(sums[-1][1]))
    out = None
    start = 0
    for index, width in enumerate(widths):
        tag = index + 1
        terms, _, own_half = sums[index]
        if tag < last:
            half_came = [block[rows:] for block in came[index]]
            halves, rest = gather_half(own_half, half_came)
            out = finish(
                out, verts, place, start, dof, inverse, white, geno_var, halves, rest, terms + came[index]
            )
        else:
            halves, rest = gather_half(own_half, last_half)
            cross, pheno_var = fit(place, inverse, white, halves, rest, terms)
            out = close(out, verts, start, dof, geno_var, pheno_var, [cross] + came[index])
        start += width
    return out


def solution(mesh):
    in_specs = (P(("grp", "subj"), None), P(("grp", "subj"), "vert"), P(("grp", "subj"), None))
    out_specs = P(("grp", "subj"), "vert")
    return jax.shard_map(associate, mesh=mesh, in_specs=in_specs, out_specs=out_specs, check_vma=False)
```

```python
import functools

import jax
import jax.numpy as jnp
from jax import lax
from jax.experimental import pallas as pl
from jax.experimental.pallas import tpu as pltpu
from jax.sharding import PartitionSpec as P


HI = lax.Precision.HIGHEST
F32 = jnp.float32
BF16 = jnp.bfloat16
LANES = 128
TILE = 512
STRIP = 256
SQUARE = 1
OPEN_LIMIT = 20 * 2**20
LIMIT = 12 * 2**20
PIECES = 4
EARLY = 2
LAST = (((1,), (1,)), ((), ()))


def round_up(value, unit):
    return -(-value // unit) * unit


def split_three(values):
    upper = values.astype(BF16)
    rest = values - upper.astype(F32)
    middle = rest.astype(BF16)
    lower = (rest - middle.astype(F32)).astype(BF16)
    return upper, middle, lower


def block_copies(source, target, sems, first, axis):
    count = PIECES if axis == 0 else max(target.shape[1] // STRIP, 1)
    step = target.shape[axis] // count
    copies = []
    for i in range(count):
        part = (slice(i * step, (i + 1) * step), slice(None))[:: 1 if axis == 0 else -1]
        copies.append(pltpu.make_async_copy(source.at[part], target.at[part], sems.at[first + i]))
    return copies


def column_block(ref, start, width):
    return ref.at[:, start : start + width]


def multiply_far(left_ref, pheno_ref, copies, give_far, keep_far, small, core, half):
    width = give_far.shape[1]
    far = give_far.shape[0] - half
    size = 2 * half
    step = min(STRIP, width) if copies else min(TILE, width)
    for low in range(0, width, step):
        high = low + step
        if copies:
            copies[low // step].wait()
        pheno = pheno_ref[:, low:high]
        result = jnp.dot(left_ref[...], pheno, preferred_element_type=F32)
        give_far[0:far, low:high] = result[:far]
        keep_far[0:far, low:high] = result[far : 2 * far]
        design = result[2 * far :]
        wide = pheno.astype(F32)
        square = jnp.sum(wide * wide, axis=0, keepdims=True)
        place = lax.broadcasted_iota(jnp.int32, (size, step), 0)
        total = (design[2 * size :] + design[size : 2 * size]) + design[:size]
        small[:, low:high] = jnp.where(place == SQUARE, square, total)
    give_far[far:, :] = small[pl.ds(pl.multiple_of((1 - core) * half, half), half), :]
    keep_far[far:, :] = small[pl.ds(pl.multiple_of(core * half, half), half), :]


def multiply_near(left_ref, pheno_ref, give_near, keep_near):
    rows, width = give_near.shape
    step = min(TILE, width)
    for low in range(0, width, step):
        result = jnp.dot(left_ref[...], pheno_ref[:, low : low + step], preferred_element_type=F32)
        give_near[:, low : low + step] = result[:rows]
        keep_near[:, low : low + step] = result[rows:]


def part_shapes(chips, rows, half, width):
    far = jax.ShapeDtypeStruct(((chips - 1) * rows + half, width), F32)
    near = jax.ShapeDtypeStruct((rows, width), F32)
    return (far, near, far, near)


def design_kernel(chips, rows, half, place_ref, left_ref, geno_ref, *refs):
    outs, (small, table) = refs[:4], refs[4:]
    give_far, give_near, keep_far, _ = outs
    chip, core = place_ref[0], place_ref[1]
    snps = geno_ref.shape[1]
    size = 2 * half
    far = (chips - 1) * size
    design = left_ref[2 * (chips - 1) * rows :, :]
    product = jnp.dot(design, geno_ref[...], preferred_element_type=F32)
    product = (product[2 * size :] + product[size : 2 * size]) + product[:size]
    wide = geno_ref[...].astype(F32)
    square = jnp.sum(wide * wide, axis=0, keepdims=True)
    row = lax.broadcasted_iota(jnp.int32, (size, snps), 0)
    product = jnp.where(row == SQUARE, square, product)
    direct = rows % LANES == 0
    if direct:
        table[...] = product
    else:
        table[...] = jnp.concatenate([product, jnp.zeros((LANES - size, snps), F32)], axis=0).T
    lanes = give_near.shape[1]
    for slot in range(chips):
        target = lax.rem(chip + slot + 1, chips) * (2 * rows)
        for side, own in ((0, 1 - core), (1, core)):
            start = pl.multiple_of(target + own * rows, rows)
            if direct:
                block = table[:, pl.ds(start, rows)]
            else:
                block = table[pl.ds(start, rows), :].T[:size]
                block = jnp.concatenate([block, jnp.zeros((size, lanes - rows), F32)], axis=1)
            if slot < chips - 1:
                outs[2 * side][slot * size : (slot + 1) * size, :] = block
            else:
                outs[2 * side + 1][...] = block
    gram = lax.dot_general(design, design, LAST, preferred_element_type=F32)
    total = jnp.zeros((size, size), F32)
    for tall, flat in ((2, 0), (0, 2), (1, 1), (1, 0), (0, 1), (0, 0)):
        total = total + gram[tall * size : (tall + 1) * size, flat * size : (flat + 1) * size]
    small[...] = jnp.concatenate([total, jnp.zeros((size, lanes - size), F32)], axis=1)
    give_far[far:, :] = small[pl.ds(pl.multiple_of((1 - core) * half, half), half), :]
    keep_far[far:, :] = small[pl.ds(pl.multiple_of(core * half, half), half), :]


def with_design(place, left, geno, chips, rows, half):
    subjects, snps = geno.shape
    lanes = round_up(rows, LANES)
    return pl.pallas_call(
        functools.partial(design_kernel, chips, rows, half),
        out_shape=part_shapes(chips, 2 * half, half, lanes),
        in_specs=[SMEM, VMEM, VMEM],
        out_specs=(VMEM,) * 4,
        scratch_shapes=[
            pltpu.VMEM((2 * half, lanes), F32),
            pltpu.VMEM((2 * half, snps) if rows % LANES == 0 else (snps, LANES), F32),
        ],
        compiler_params=pltpu.CompilerParams(vmem_limit_bytes=LIMIT),
        cost_estimate=cost(2 * 6 * half * subjects * snps, 2 * subjects * snps),
        name="with_design",
    )(place, left, geno)


def open_kernel(chips, rows, half, place_ref, geno_ref, cov_ref, pheno_ref, *refs):
    left_ref, geno, give_far, keep_far = refs[:4]
    heres, (turned, design, small, sems) = refs[4:-4], refs[-4:]
    chip, core = place_ref[0], place_ref[1]
    covs, subjects = cov_ref.shape
    far = (chips - 1) * rows
    size = 2 * half
    cov_copy = pltpu.make_async_copy(cov_ref, design.at[8 : 8 + covs], sems.at[0])
    cov_copy.start()
    geno_copies = block_copies(geno_ref, geno, sems, 1, 0)
    first = heres[0]
    first_copies = block_copies(column_block(pheno_ref, 0, first.shape[1]), first, sems, 1 + PIECES, 1)
    for copy in geno_copies + first_copies:
        copy.start()
    used, start = 1 + PIECES + len(first_copies), first.shape[1]
    later_copies = []
    for here in heres[1:]:
        later_copies += block_copies(column_block(pheno_ref, start, here.shape[1]), here, sems, used, 0)
        used, start = used + PIECES, start + here.shape[1]
    top = lax.broadcasted_iota(jnp.int32, (8, subjects), 0)
    design[0:8, :] = jnp.where(top == 0, 1.0, 0.0)
    if size > 8 + covs:
        design[8 + covs :, :] = jnp.zeros((size - 8 - covs, subjects), F32)
    cov_copy.wait()
    for index, part in enumerate(split_three(design[...])):
        left_ref[2 * far + index * size : 2 * far + (index + 1) * size, :] = part
    step = subjects // PIECES
    direct = 2 * rows % LANES == 0
    for index, copy in enumerate(geno_copies):
        copy.wait()
        low, high = index * step, (index + 1) * step
        if direct:
            for slot in range(chips - 1):
                target = pl.multiple_of(lax.rem(chip + slot + 1, chips) * (2 * rows), 2 * rows)
                base = slot * 2 * rows
                turned[base : base + 2 * rows, low:high] = geno[low:high, pl.ds(target, 2 * rows)].T
        else:
            turned[:, low:high] = geno[low:high, :].T
    for copy in later_copies:
        copy.start()
    for slot in range(chips - 1):
        target = slot * 2 * rows if direct else lax.rem(chip + slot + 1, chips) * (2 * rows)
        for side, own in ((0, 1 - core), (1, core)):
            low = side * far + slot * rows
            left_ref[low : low + rows, :] = turned[pl.ds(pl.multiple_of(target + own * rows, rows), rows), :]
    multiply_far(left_ref, first, first_copies, give_far, keep_far, small, core, half)
    for copy in later_copies:
        copy.wait()


def near_kernel(rows, start, early, place_ref, geno_ref, pheno_ref, *refs):
    heres, left_ref, outs = refs[:early], refs[early], refs[early + 1 : 3 * early + 1]
    later, (turned, sems) = refs[3 * early + 1 : -2], refs[-2:]
    chip, core = place_ref[0], place_ref[1]
    copies = []
    for target in later:
        copies += block_copies(column_block(pheno_ref, start, target.shape[1]), target, sems, 0, 0)
    for copy in copies:
        copy.start()

    @pl.when(core >= 0)
    def _():
        if 2 * rows % LANES == 0:
            turned[0 : 2 * rows, :] = geno_ref[:, pl.ds(pl.multiple_of(chip * (2 * rows), 2 * rows), 2 * rows)].T
            base = 0
        else:
            turned[...] = geno_ref[...].T
            base = chip * (2 * rows)
        for side, own in ((0, 1 - core), (1, core)):
            low = pl.multiple_of(base + own * rows, rows)
            left_ref[side * rows : (side + 1) * rows, :] = turned[pl.ds(low, rows), :]
        for index, here in enumerate(heres):
            multiply_near(left_ref, here, outs[2 * index], outs[2 * index + 1])

    for copy in copies:
        copy.wait()


def cost(flops, moved):
    return pl.CostEstimate(flops=flops, bytes_accessed=moved, transcendentals=0)


def in_hbm(array):
    return pltpu.with_memory_space_constraint(array, pltpu.HBM)


SMEM = pl.BlockSpec(memory_space=pltpu.SMEM)
VMEM = pl.BlockSpec(memory_space=pltpu.VMEM)
HBM = pl.BlockSpec(memory_space=pltpu.HBM)


def open_up(place, dosage, cov_rows, phenotype, chips, rows, half, widths):
    subjects, snps = dosage.shape
    width = widths[0]
    height = 2 * (chips - 1) * rows + 6 * half
    left = jax.ShapeDtypeStruct((height, subjects), BF16)
    geno = jax.ShapeDtypeStruct((subjects, snps), BF16)
    heres = [jax.ShapeDtypeStruct((subjects, size), BF16) for size in widths]
    part = part_shapes(chips, rows, half, width)[0]
    return pl.pallas_call(
        functools.partial(open_kernel, chips, rows, half),
        out_shape=(left, geno, part, part, *heres),
        in_specs=[SMEM, HBM, HBM, HBM],
        out_specs=(VMEM,) * (4 + len(heres)),
        scratch_shapes=[
            pltpu.VMEM((snps, subjects), BF16),
            pltpu.VMEM((2 * half, subjects), F32),
            pltpu.VMEM((2 * half, width), F32),
            pltpu.SemaphoreType.DMA((1 + len(heres) * PIECES + max(width // STRIP, 1),)),
        ],
        compiler_params=pltpu.CompilerParams(vmem_limit_bytes=OPEN_LIMIT),
        cost_estimate=cost(2 * height * subjects * width, 4 * snps * subjects),
        name="open",
    )(place, in_hbm(dosage), in_hbm(cov_rows), in_hbm(phenotype))


def open_near(place, geno, heres, phenotype, later, rows):
    subjects, snps = geno.shape
    widths = [here.shape[1] for here in heres]
    parts = [jax.ShapeDtypeStruct((rows, width), F32) for width in widths for _ in range(2)]
    left = jax.ShapeDtypeStruct((2 * rows, subjects), BF16)
    ahead = [jax.ShapeDtypeStruct((subjects, size), BF16) for size in later]
    return pl.pallas_call(
        functools.partial(near_kernel, rows, sum(widths), len(heres)),
        out_shape=(left, *parts, *ahead),
        in_specs=[SMEM, VMEM, HBM] + [VMEM] * len(heres),
        out_specs=(VMEM,) * (1 + len(parts) + len(ahead)),
        scratch_shapes=[pltpu.VMEM((snps, subjects), BF16), pltpu.SemaphoreType.DMA((PIECES,))],
        compiler_params=pltpu.CompilerParams(vmem_limit_bytes=LIMIT),
        cost_estimate=cost(4 * rows * subjects * sum(widths), 4 * snps * subjects),
        name="open_near",
    )(place, geno, in_hbm(phenotype), *heres)


def far_kernel(half, place_ref, far_ref, here_ref, give_far, keep_far, small):
    multiply_far(far_ref, here_ref, [], give_far, keep_far, small, place_ref[1], half)


def far_product(place, left, here, chips, rows, half):
    height, subjects = left.shape
    width = here.shape[1]
    part = part_shapes(chips, rows, half, width)[0]
    return pl.pallas_call(
        functools.partial(far_kernel, half),
        out_shape=(part, part),
        in_specs=[SMEM, VMEM, VMEM],
        out_specs=(VMEM, VMEM),
        scratch_shapes=[pltpu.VMEM((2 * half, width), F32)],
        compiler_params=pltpu.CompilerParams(vmem_limit_bytes=LIMIT),
        cost_estimate=cost(2 * height * subjects * width, 2 * subjects * width),
    )(place, left, here)


def product_kernel(half, start, place_ref, far_ref, near_ref, here_ref, pheno_ref, *refs):
    give_far, give_near, keep_far, keep_near = refs[:4]
    later, (small, sems) = refs[4:-2], refs[-2:]
    core = place_ref[1]
    copies = []
    for target in later:
        copies += block_copies(column_block(pheno_ref, start, target.shape[1]), target, sems, 0, 0)
    for copy in copies:
        copy.start()

    @pl.when(core >= 0)
    def _():
        multiply_far(far_ref, here_ref, [], give_far, keep_far, small, core, half)
        multiply_near(near_ref, here_ref, give_near, keep_near)

    for copy in copies:
        copy.wait()


def product(place, left, near, here, phenotype, start, later, chips, rows, half):
    height, subjects = left.shape
    width = here.shape[1]
    ahead = [jax.ShapeDtypeStruct((subjects, size), BF16) for size in later]
    return pl.pallas_call(
        functools.partial(product_kernel, half, start + width),
        out_shape=(*part_shapes(chips, rows, half, width), *ahead),
        in_specs=[SMEM, VMEM, VMEM, VMEM, HBM],
        out_specs=(VMEM,) * (4 + len(ahead)),
        scratch_shapes=[pltpu.VMEM((2 * half, width), F32), pltpu.SemaphoreType.DMA((PIECES,))],
        compiler_params=pltpu.CompilerParams(vmem_limit_bytes=LIMIT),
        cost_estimate=cost(2 * (height + 2 * rows) * subjects * width, 2 * subjects * width),
    )(place, left, near, here, in_hbm(phenotype))


def solve_kernel(live, half, count, *refs):
    place_ref, half_ref, rest_ref = refs[:3]
    terms, (inverse_ref, white_ref, var_ref, work) = refs[3 : 3 + count], refs[3 + count :]
    core = place_ref[1]
    size = 2 * half
    work[pl.ds(pl.multiple_of(core * half, half), half), :] = half_ref[...]
    work[pl.ds(pl.multiple_of((1 - core) * half, half), half), :] = rest_ref[...]
    row = lax.broadcasted_iota(jnp.int32, (size, LANES), 0)
    lane = lax.broadcasted_iota(jnp.int32, (size, LANES), 1)
    left = jnp.where(lane < size, work[...], 0.0)
    right = jnp.where(lane == row, 1.0, 0.0)
    scaled = jnp.zeros((size, LANES), F32)
    for step in live:
        pivot = jnp.broadcast_to(left[:, step : step + 1], (size, LANES))
        top = jnp.broadcast_to(pivot[step : step + 1], (size, LANES))
        ratio = jnp.where(row > step, pivot / top, 0.0)
        root = lax.rsqrt(top)
        root = root * (1.5 - 0.5 * top * root * root)
        scaled = jnp.where(row == step, right * root, scaled)
        left = left - ratio * left[step : step + 1]
        right = right - ratio * right[step : step + 1]
    inverse_ref[...] = scaled
    own = terms[0][...]
    for term in terms[1:]:
        own = own + term[...]
    rows = white_ref.shape[0]
    white = jnp.dot(scaled[:, :size], own, precision=HI, preferred_element_type=F32)
    geno_var = own[SQUARE : SQUARE + 1] - jnp.sum(white * white, axis=0, keepdims=True)
    white = jnp.concatenate([white, jnp.zeros((LANES - size, own.shape[1]), F32)], axis=0)
    white_ref[...] = white.T[:rows]
    var_ref[...] = jnp.broadcast_to(geno_var, (LANES, own.shape[1])).T[:rows]


def solve(place, half_rows, rest_rows, terms, live, rows):
    half = half_rows.shape[0]
    wide = jax.ShapeDtypeStruct((rows, LANES), F32)
    return pl.pallas_call(
        functools.partial(solve_kernel, live, half, len(terms)),
        out_shape=(jax.ShapeDtypeStruct((2 * half, LANES), F32), wide, wide),
        in_specs=[SMEM] + [VMEM] * (2 + len(terms)),
        out_specs=(VMEM,) * 3,
        scratch_shapes=[pltpu.VMEM((2 * half, LANES), F32)],
        compiler_params=pltpu.CompilerParams(vmem_limit_bytes=LIMIT),
        cost_estimate=cost(5 * 10**9, 2**16),
        name="solve",
    )(place, half_rows, rest_rows, *terms)


def finish_kernel(dof, count, *refs):
    place_ref, inverse_ref, white_ref, var_ref, half_ref, rest_ref = refs[:6]
    terms, out_ref, small = refs[6 : 6 + count], refs[-2], refs[-1]
    half = half_ref.shape[0]
    rows, tile = out_ref.shape
    core = place_ref[1]
    low = pl.multiple_of(pl.program_id(0) * tile, tile)
    small[pl.ds(pl.multiple_of(core * half, half), half), :] = half_ref[:, pl.ds(low, tile)]
    small[pl.ds(pl.multiple_of((1 - core) * half, half), half), :] = rest_ref[:, pl.ds(low, tile)]
    white = jnp.dot(inverse_ref[:, : 2 * half], small[...], precision=HI, preferred_element_type=F32)
    pheno_var = small[SQUARE : SQUARE + 1, :] - jnp.sum(white * white, axis=0, keepdims=True)
    fitted = jnp.dot(white_ref[:, : 2 * half], white, precision=HI, preferred_element_type=F32)
    cross = terms[0][0:rows, pl.ds(low, tile)]
    for term in terms[1:]:
        cross = cross + term[0:rows, pl.ds(low, tile)]
    cross = cross - fitted
    out_ref[...] = cross * dof * lax.rsqrt(var_ref[:, 0:1] * pheno_var - cross * cross)


def finish(done, total, place, start, dof, inverse, white, geno_var, half_rows, rest_rows, terms):
    rows, width = terms[0].shape
    tile = min(TILE, width)
    first = start // tile
    args = [place, inverse, white, geno_var, half_rows, rest_rows, *terms]
    specs = [SMEM] + [VMEM] * (len(args) - 1)
    aliases = {}
    if done is not None:
        aliases = {len(args): 0}
        args.append(done)
        specs.append(HBM)
    return pl.pallas_call(
        functools.partial(finish_kernel, dof, len(terms)),
        grid=(width // tile,),
        out_shape=jax.ShapeDtypeStruct((rows, total), F32),
        in_specs=specs,
        out_specs=pl.BlockSpec((rows, tile), lambda j: (0, first + j)),
        scratch_shapes=[pltpu.VMEM((2 * half_rows.shape[0], tile), F32)],
        input_output_aliases=aliases,
        compiler_params=pltpu.CompilerParams(vmem_limit_bytes=LIMIT),
        cost_estimate=pl.CostEstimate(
            flops=2 * 256 * 256 * width, bytes_accessed=16 * rows * width, transcendentals=rows * width
        ),
    )(*args)


def fit_kernel(count, *refs):
    place_ref, inverse_ref, white_ref, half_ref, rest_ref = refs[:5]
    terms, (cross_ref, var_ref, small) = refs[5 : 5 + count], refs[5 + count :]
    half = half_ref.shape[0]
    core = place_ref[1]
    small[pl.ds(pl.multiple_of(core * half, half), half), :] = half_ref[...]
    small[pl.ds(pl.multiple_of((1 - core) * half, half), half), :] = rest_ref[...]
    white = jnp.dot(inverse_ref[:, : 2 * half], small[...], precision=HI, preferred_element_type=F32)
    pheno_var = small[SQUARE : SQUARE + 1, :] - jnp.sum(white * white, axis=0, keepdims=True)
    var_ref[...] = jnp.broadcast_to(pheno_var, var_ref.shape)
    fitted = jnp.dot(white_ref[:, : 2 * half], white, precision=HI, preferred_element_type=F32)
    cross = terms[0][...]
    for term in terms[1:]:
        cross = cross + term[...]
    cross_ref[...] = cross - fitted


def fit(place, inverse, white, half_rows, rest_rows, terms):
    rows, width = terms[0].shape
    args = [place, inverse, white, half_rows, rest_rows, *terms]
    return pl.pallas_call(
        functools.partial(fit_kernel, len(terms)),
        out_shape=(jax.ShapeDtypeStruct((rows, width), F32), jax.ShapeDtypeStruct((8, width), F32)),
        in_specs=[SMEM] + [VMEM] * (len(args) - 1),
        out_specs=(VMEM, VMEM),
        scratch_shapes=[pltpu.VMEM((2 * half_rows.shape[0], width), F32)],
        compiler_params=pltpu.CompilerParams(vmem_limit_bytes=LIMIT),
        cost_estimate=cost(2 * 256 * 256 * width, 16 * rows * width),
        name="fit",
    )(*args)


def close_kernel(dof, count, *refs):
    geno_var_ref, pheno_var_ref = refs[:2]
    terms, out_ref = refs[2 : 2 + count], refs[-1]
    tile = out_ref.shape[1]
    low = pl.multiple_of(pl.program_id(0) * tile, tile)
    cross = terms[0][:, pl.ds(low, tile)]
    for term in terms[1:]:
        cross = cross + term[:, pl.ds(low, tile)]
    pheno_var = pheno_var_ref[0:1, pl.ds(low, tile)]
    out_ref[...] = cross * dof * lax.rsqrt(geno_var_ref[:, 0:1] * pheno_var - cross * cross)


def close(done, total, start, dof, geno_var, pheno_var, terms):
    rows, width = terms[0].shape
    tile = min(STRIP, width)
    first = start // tile
    args = [geno_var, pheno_var, *terms]
    specs = [VMEM] * len(args)
    aliases = {}
    if done is not None:
        aliases = {len(args): 0}
        args.append(done)
        specs.append(HBM)
    return pl.pallas_call(
        functools.partial(close_kernel, dof, len(terms)),
        grid=(width // tile,),
        out_shape=jax.ShapeDtypeStruct((rows, total), F32),
        in_specs=specs,
        out_specs=pl.BlockSpec((rows, tile), lambda j: (0, first + j)),
        input_output_aliases=aliases,
        compiler_params=pltpu.CompilerParams(vmem_limit_bytes=LIMIT),
        cost_estimate=cost(8 * rows * width, 12 * rows * width),
        name="close",
    )(*args)


def chunk_widths(total):
    units = total // TILE
    if total % TILE or units < 2:
        return [total]
    wide, odd = divmod(max(units - 4, 0), 2)
    sizes = [1] * min(units - units // 2, 2) + [2] * wide + [1] * odd + [1] * min(units // 2, 2)
    return [size * TILE for size in sizes]


def associate(dosage, phenotype, covariates):
    devices = lax.axis_size("subj")
    chips = devices // 2
    subjects, snps = dosage.shape
    verts = phenotype.shape[1]
    covs = covariates.shape[1]
    rows = snps // devices
    half = round_up(8 + covs, 16) // 2
    live = [0] + list(range(8, 8 + covs))
    place_index = lax.axis_index("subj")
    place = jnp.stack([place_index // 2, lax.rem(place_index, 2)]).astype(jnp.int32)
    sibling = [(i, i ^ 1) for i in range(devices)]

    def far_got(give_far):
        return lax.ppermute(give_far, "subj", sibling)

    def near_sums(parts, apart=False, got_far=None, unit=rows):
        far = (chips - 1) * unit
        give_far, give_near, keep_far, keep_near = parts
        if got_far is None:
            got_far = far_got(give_far)
        got_near = lax.ppermute(give_near, "subj", sibling)
        terms = [keep_near, got_near]
        if apart:
            blocks = [keep_far[low : low + unit] + got_far[low : low + unit] for low in range(0, far, unit)]
            return terms, blocks, keep_far[far:] + got_far[far:]
        summed = keep_far + got_far
        if chips == 2:
            return terms, [summed], summed[unit:]
        own_half = summed[far:]
        blocks = [jnp.concatenate([summed[low : low + unit], own_half], axis=0) for low in range(0, far, unit)]
        return terms, blocks, own_half

    def far_terms(blocks):
        came = []
        for step, block in enumerate(blocks, 1):
            moves = [(i, (i + 2 * step) % devices) for i in range(devices)]
            came.append(lax.ppermute(block, "subj", moves))
        return came

    def gather_half(halves, came):
        for block in came:
            halves = halves + block
        rest = lax.ppermute(halves, "subj", sibling)
        return halves, rest

    widths = chunk_widths(verts)
    last = len(widths)
    early = widths[:EARLY]
    left, geno, give_far, keep_far, *heres = open_up(place, dosage, covariates.T, phenotype, chips, rows, half, early)
    fars = [(give_far, keep_far, far_got(give_far))]
    for index in range(1, len(early)):
        give_far, keep_far = far_product(place, left, heres[index], chips, rows, half)
        fars.append((give_far, keep_far, far_got(give_far)))
    near, *nears = open_near(place, geno, heres, phenotype, widths[EARLY : EARLY + 1], rows)
    ahead = nears[2 * len(early) :]
    sums, came = [], []
    for index, (give_far, keep_far, got_far) in enumerate(fars):
        give_near, keep_near = nears[2 * index : 2 * index + 2]
        sums.append(near_sums((give_far, give_near, keep_far, keep_near), got_far=got_far))
        came.append(far_terms(sums[-1][1]))
    parts = with_design(place, left, geno, chips, rows, half)
    terms, blocks, own_half = near_sums(parts, unit=2 * half)
    base_came = far_terms(blocks)
    halves, rest = gather_half(own_half, [block[2 * half :] for block in base_came])
    inverse, white, geno_var = solve(
        place, halves, rest, terms + [block[: 2 * half] for block in base_came], live, rows
    )
    dof = float(subjects * devices - covs - 2) ** 0.5

    start = sum(early)
    for index in range(EARLY, last):
        tag = index + 1
        parts = product(place, left, near, ahead[0], phenotype, start, widths[index + 1 : index + 2], chips, rows, half)
        ahead = parts[4:]
        start += widths[index]
        sums.append(near_sums(parts[:4], apart=tag == last))
        if tag == last:
            last_half = far_terms([sums[-1][2]] * (chips - 1))
        came.append(far_terms(sums[-1][1]))
    out = None
    start = 0
    for index, width in enumerate(widths):
        tag = index + 1
        terms, _, own_half = sums[index]
        if tag < last:
            half_came = [block[rows:] for block in came[index]]
            halves, rest = gather_half(own_half, half_came)
            out = finish(
                out, verts, place, start, dof, inverse, white, geno_var, halves, rest, terms + came[index]
            )
        else:
            halves, rest = gather_half(own_half, last_half)
            cross, pheno_var = fit(place, inverse, white, halves, rest, terms)
            out = close(out, verts, start, dof, geno_var, pheno_var, [cross] + came[index])
        start += width
    return out


def solution(mesh):
    in_specs = (P(("grp", "subj"), None), P(("grp", "subj"), "vert"), P(("grp", "subj"), None))
    out_specs = P(("grp", "subj"), "vert")
    return jax.shard_map(associate, mesh=mesh, in_specs=in_specs, out_specs=out_specs, check_vma=False)
```

```python
import functools

import jax
import jax.numpy as jnp
from jax import lax
from jax.experimental import pallas as pl
from jax.experimental.pallas import tpu as pltpu
from jax.sharding import PartitionSpec as P


HI = lax.Precision.HIGHEST
F32 = jnp.float32
BF16 = jnp.bfloat16
LANES = 128
TILE = 512
STRIP = 256
SQUARE = 1
OPEN_LIMIT = 20 * 2**20
LIMIT = 12 * 2**20
PIECES = 4
EARLY = 2
LAST = (((1,), (1,)), ((), ()))


def round_up(value, unit):
    return -(-value // unit) * unit


def split_three(values):
    upper = values.astype(BF16)
    rest = values - upper.astype(F32)
    middle = rest.astype(BF16)
    lower = (rest - middle.astype(F32)).astype(BF16)
    return upper, middle, lower


def block_copies(source, target, sems, first, axis):
    count = PIECES if axis == 0 else max(target.shape[1] // STRIP, 1)
    step = target.shape[axis] // count
    copies = []
    for i in range(count):
        part = (slice(i * step, (i + 1) * step), slice(None))[:: 1 if axis == 0 else -1]
        copies.append(pltpu.make_async_copy(source.at[part], target.at[part], sems.at[first + i]))
    return copies


def column_block(ref, start, width):
    return ref.at[:, start : start + width]


def multiply_far(left_ref, pheno_ref, copies, give_far, keep_far, small, core, half):
    width = give_far.shape[1]
    far = give_far.shape[0] - half
    size = 2 * half
    step = min(STRIP, width) if copies else min(TILE, width)
    for low in range(0, width, step):
        high = low + step
        if copies:
            copies[low // step].wait()
        pheno = pheno_ref[:, low:high]
        result = jnp.dot(left_ref[...], pheno, preferred_element_type=F32)
        give_far[0:far, low:high] = result[:far]
        keep_far[0:far, low:high] = result[far : 2 * far]
        design = result[2 * far :]
        wide = pheno.astype(F32)
        square = jnp.sum(wide * wide, axis=0, keepdims=True)
        place = lax.broadcasted_iota(jnp.int32, (size, step), 0)
        total = (design[2 * size :] + design[size : 2 * size]) + design[:size]
        small[:, low:high] = jnp.where(place == SQUARE, square, total)
    give_far[far:, :] = small[pl.ds(pl.multiple_of((1 - core) * half, half), half), :]
    keep_far[far:, :] = small[pl.ds(pl.multiple_of(core * half, half), half), :]


def multiply_near(left_ref, pheno_ref, give_near, keep_near):
    rows, width = give_near.shape
    step = min(TILE, width)
    for low in range(0, width, step):
        result = jnp.dot(left_ref[...], pheno_ref[:, low : low + step], preferred_element_type=F32)
        give_near[:, low : low + step] = result[:rows]
        keep_near[:, low : low + step] = result[rows:]


def part_shapes(chips, rows, half, width):
    far = jax.ShapeDtypeStruct(((chips - 1) * rows + half, width), F32)
    near = jax.ShapeDtypeStruct((rows, width), F32)
    return (far, near, far, near)


def design_kernel(chips, rows, half, place_ref, left_ref, geno_ref, *refs):
    outs, (small, table) = refs[:4], refs[4:]
    give_far, give_near, keep_far, _ = outs
    chip, core = place_ref[0], place_ref[1]
    snps = geno_ref.shape[1]
    size = 2 * half
    far = (chips - 1) * size
    design = left_ref[2 * (chips - 1) * rows :, :]
    product = jnp.dot(design, geno_ref[...], preferred_element_type=F32)
    product = (product[2 * size :] + product[size : 2 * size]) + product[:size]
    wide = geno_ref[...].astype(F32)
    square = jnp.sum(wide * wide, axis=0, keepdims=True)
    row = lax.broadcasted_iota(jnp.int32, (size, snps), 0)
    product = jnp.where(row == SQUARE, square, product)
    direct = rows % LANES == 0
    if direct:
        table[...] = product
    else:
        table[...] = jnp.concatenate([product, jnp.zeros((LANES - size, snps), F32)], axis=0).T
    lanes = give_near.shape[1]
    for slot in range(chips):
        target = lax.rem(chip + slot + 1, chips) * (2 * rows)
        for side, own in ((0, 1 - core), (1, core)):
            start = pl.multiple_of(target + own * rows, rows)
            if direct:
                block = table[:, pl.ds(start, rows)]
            else:
                block = table[pl.ds(start, rows), :].T[:size]
                block = jnp.concatenate([block, jnp.zeros((size, lanes - rows), F32)], axis=1)
            if slot < chips - 1:
                outs[2 * side][slot * size : (slot + 1) * size, :] = block
            else:
                outs[2 * side + 1][...] = block
    gram = lax.dot_general(design, design, LAST, preferred_element_type=F32)
    total = jnp.zeros((size, size), F32)
    for tall, flat in ((2, 0), (0, 2), (1, 1), (1, 0), (0, 1), (0, 0)):
        total = total + gram[tall * size : (tall + 1) * size, flat * size : (flat + 1) * size]
    small[...] = jnp.concatenate([total, jnp.zeros((size, lanes - size), F32)], axis=1)
    give_far[far:, :] = small[pl.ds(pl.multiple_of((1 - core) * half, half), half), :]
    keep_far[far:, :] = small[pl.ds(pl.multiple_of(core * half, half), half), :]


def with_design(place, left, geno, chips, rows, half):
    subjects, snps = geno.shape
    lanes = round_up(rows, LANES)
    return pl.pallas_call(
        functools.partial(design_kernel, chips, rows, half),
        out_shape=part_shapes(chips, 2 * half, half, lanes),
        in_specs=[SMEM, VMEM, VMEM],
        out_specs=(VMEM,) * 4,
        scratch_shapes=[
            pltpu.VMEM((2 * half, lanes), F32),
            pltpu.VMEM((2 * half, snps) if rows % LANES == 0 else (snps, LANES), F32),
        ],
        compiler_params=pltpu.CompilerParams(vmem_limit_bytes=LIMIT),
        cost_estimate=cost(2 * 6 * half * subjects * snps, 2 * subjects * snps),
        name="with_design",
    )(place, left, geno)


def open_kernel(chips, rows, half, place_ref, geno_ref, cov_ref, pheno_ref, *refs):
    left_ref, geno, give_far, keep_far = refs[:4]
    heres, (turned, design, small, sems) = refs[4:-4], refs[-4:]
    chip, core = place_ref[0], place_ref[1]
    covs, subjects = cov_ref.shape
    far = (chips - 1) * rows
    size = 2 * half
    cov_copy = pltpu.make_async_copy(cov_ref, design.at[8 : 8 + covs], sems.at[0])
    cov_copy.start()
    geno_copies = block_copies(geno_ref, geno, sems, 1, 0)
    first = heres[0]
    first_copies = block_copies(column_block(pheno_ref, 0, first.shape[1]), first, sems, 1 + PIECES, 1)
    for copy in geno_copies + first_copies:
        copy.start()
    used, start = 1 + PIECES + len(first_copies), first.shape[1]
    later_copies = []
    for here in heres[1:]:
        later_copies += block_copies(column_block(pheno_ref, start, here.shape[1]), here, sems, used, 0)
        used, start = used + PIECES, start + here.shape[1]
    top = lax.broadcasted_iota(jnp.int32, (8, subjects), 0)
    design[0:8, :] = jnp.where(top == 0, 1.0, 0.0)
    if size > 8 + covs:
        design[8 + covs :, :] = jnp.zeros((size - 8 - covs, subjects), F32)
    cov_copy.wait()
    for index, part in enumerate(split_three(design[...])):
        left_ref[2 * far + index * size : 2 * far + (index + 1) * size, :] = part
    step = subjects // PIECES
    direct = 2 * rows % LANES == 0
    for copy in geno_copies:
        copy.wait()
    for index in range(PIECES):
        low, high = index * step, (index + 1) * step
        if direct:
            for slot in range(chips - 1):
                target = pl.multiple_of(lax.rem(chip + slot + 1, chips) * (2 * rows), 2 * rows)
                base = slot * 2 * rows
                turned[base : base + 2 * rows, low:high] = geno[low:high, pl.ds(target, 2 * rows)].T
        else:
            turned[:, low:high] = geno[low:high, :].T
    for copy in later_copies:
        copy.start()
    for slot in range(chips - 1):
        target = slot * 2 * rows if direct else lax.rem(chip + slot + 1, chips) * (2 * rows)
        for side, own in ((0, 1 - core), (1, core)):
            low = side * far + slot * rows
            left_ref[low : low + rows, :] = turned[pl.ds(pl.multiple_of(target + own * rows, rows), rows), :]
    for copy in first_copies:
        copy.wait()
    multiply_far(left_ref, first, [], give_far, keep_far, small, core, half)
    for copy in later_copies:
        copy.wait()


def near_kernel(rows, start, early, place_ref, geno_ref, pheno_ref, *refs):
    heres, left_ref, outs = refs[:early], refs[early], refs[early + 1 : 3 * early + 1]
    later, (turned, sems) = refs[3 * early + 1 : -2], refs[-2:]
    chip, core = place_ref[0], place_ref[1]
    copies = []
    for target in later:
        copies += block_copies(column_block(pheno_ref, start, target.shape[1]), target, sems, 0, 0)
    for copy in copies:
        copy.start()

    @pl.when(core >= 0)
    def _():
        if 2 * rows % LANES == 0:
            turned[0 : 2 * rows, :] = geno_ref[:, pl.ds(pl.multiple_of(chip * (2 * rows), 2 * rows), 2 * rows)].T
            base = 0
        else:
            turned[...] = geno_ref[...].T
            base = chip * (2 * rows)
        for side, own in ((0, 1 - core), (1, core)):
            low = pl.multiple_of(base + own * rows, rows)
            left_ref[side * rows : (side + 1) * rows, :] = turned[pl.ds(low, rows), :]
        for index, here in enumerate(heres):
            multiply_near(left_ref, here, outs[2 * index], outs[2 * index + 1])

    for copy in copies:
        copy.wait()


def cost(flops, moved):
    return pl.CostEstimate(flops=flops, bytes_accessed=moved, transcendentals=0)


def in_hbm(array):
    return pltpu.with_memory_space_constraint(array, pltpu.HBM)


SMEM = pl.BlockSpec(memory_space=pltpu.SMEM)
VMEM = pl.BlockSpec(memory_space=pltpu.VMEM)
HBM = pl.BlockSpec(memory_space=pltpu.HBM)


def open_up(place, dosage, cov_rows, phenotype, chips, rows, half, widths):
    subjects, snps = dosage.shape
    width = widths[0]
    height = 2 * (chips - 1) * rows + 6 * half
    left = jax.ShapeDtypeStruct((height, subjects), BF16)
    geno = jax.ShapeDtypeStruct((subjects, snps), BF16)
    heres = [jax.ShapeDtypeStruct((subjects, size), BF16) for size in widths]
    part = part_shapes(chips, rows, half, width)[0]
    return pl.pallas_call(
        functools.partial(open_kernel, chips, rows, half),
        out_shape=(left, geno, part, part, *heres),
        in_specs=[SMEM, HBM, HBM, HBM],
        out_specs=(VMEM,) * (4 + len(heres)),
        scratch_shapes=[
            pltpu.VMEM((snps, subjects), BF16),
            pltpu.VMEM((2 * half, subjects), F32),
            pltpu.VMEM((2 * half, width), F32),
            pltpu.SemaphoreType.DMA((1 + len(heres) * PIECES + max(width // STRIP, 1),)),
        ],
        compiler_params=pltpu.CompilerParams(vmem_limit_bytes=OPEN_LIMIT),
        cost_estimate=cost(2 * height * subjects * width, 4 * snps * subjects),
        name="open",
    )(place, in_hbm(dosage), in_hbm(cov_rows), in_hbm(phenotype))


def open_near(place, geno, heres, phenotype, later, rows):
    subjects, snps = geno.shape
    widths = [here.shape[1] for here in heres]
    parts = [jax.ShapeDtypeStruct((rows, width), F32) for width in widths for _ in range(2)]
    left = jax.ShapeDtypeStruct((2 * rows, subjects), BF16)
    ahead = [jax.ShapeDtypeStruct((subjects, size), BF16) for size in later]
    return pl.pallas_call(
        functools.partial(near_kernel, rows, sum(widths), len(heres)),
        out_shape=(left, *parts, *ahead),
        in_specs=[SMEM, VMEM, HBM] + [VMEM] * len(heres),
        out_specs=(VMEM,) * (1 + len(parts) + len(ahead)),
        scratch_shapes=[pltpu.VMEM((snps, subjects), BF16), pltpu.SemaphoreType.DMA((PIECES,))],
        compiler_params=pltpu.CompilerParams(vmem_limit_bytes=LIMIT),
        cost_estimate=cost(4 * rows * subjects * sum(widths), 4 * snps * subjects),
        name="open_near",
    )(place, geno, in_hbm(phenotype), *heres)


def far_kernel(half, place_ref, far_ref, here_ref, give_far, keep_far, small):
    multiply_far(far_ref, here_ref, [], give_far, keep_far, small, place_ref[1], half)


def far_product(place, left, here, chips, rows, half):
    height, subjects = left.shape
    width = here.shape[1]
    part = part_shapes(chips, rows, half, width)[0]
    return pl.pallas_call(
        functools.partial(far_kernel, half),
        out_shape=(part, part),
        in_specs=[SMEM, VMEM, VMEM],
        out_specs=(VMEM, VMEM),
        scratch_shapes=[pltpu.VMEM((2 * half, width), F32)],
        compiler_params=pltpu.CompilerParams(vmem_limit_bytes=LIMIT),
        cost_estimate=cost(2 * height * subjects * width, 2 * subjects * width),
    )(place, left, here)


def product_kernel(half, start, place_ref, far_ref, near_ref, here_ref, pheno_ref, *refs):
    give_far, give_near, keep_far, keep_near = refs[:4]
    later, (small, sems) = refs[4:-2], refs[-2:]
    core = place_ref[1]
    copies = []
    for target in later:
        copies += block_copies(column_block(pheno_ref, start, target.shape[1]), target, sems, 0, 0)
    for copy in copies:
        copy.start()

    @pl.when(core >= 0)
    def _():
        multiply_far(far_ref, here_ref, [], give_far, keep_far, small, core, half)
        multiply_near(near_ref, here_ref, give_near, keep_near)

    for copy in copies:
        copy.wait()


def product(place, left, near, here, phenotype, start, later, chips, rows, half):
    height, subjects = left.shape
    width = here.shape[1]
    ahead = [jax.ShapeDtypeStruct((subjects, size), BF16) for size in later]
    return pl.pallas_call(
        functools.partial(product_kernel, half, start + width),
        out_shape=(*part_shapes(chips, rows, half, width), *ahead),
        in_specs=[SMEM, VMEM, VMEM, VMEM, HBM],
        out_specs=(VMEM,) * (4 + len(ahead)),
        scratch_shapes=[pltpu.VMEM((2 * half, width), F32), pltpu.SemaphoreType.DMA((PIECES,))],
        compiler_params=pltpu.CompilerParams(vmem_limit_bytes=LIMIT),
        cost_estimate=cost(2 * (height + 2 * rows) * subjects * width, 2 * subjects * width),
    )(place, left, near, here, in_hbm(phenotype))


def solve_kernel(live, half, count, *refs):
    place_ref, half_ref, rest_ref = refs[:3]
    terms, (inverse_ref, white_ref, var_ref, work) = refs[3 : 3 + count], refs[3 + count :]
    core = place_ref[1]
    size = 2 * half
    work[pl.ds(pl.multiple_of(core * half, half), half), :] = half_ref[...]
    work[pl.ds(pl.multiple_of((1 - core) * half, half), half), :] = rest_ref[...]
    row = lax.broadcasted_iota(jnp.int32, (size, LANES), 0)
    lane = lax.broadcasted_iota(jnp.int32, (size, LANES), 1)
    left = jnp.where(lane < size, work[...], 0.0)
    right = jnp.where(lane == row, 1.0, 0.0)
    scaled = jnp.zeros((size, LANES), F32)
    for step in live:
        pivot = jnp.broadcast_to(left[:, step : step + 1], (size, LANES))
        top = jnp.broadcast_to(pivot[step : step + 1], (size, LANES))
        ratio = jnp.where(row > step, pivot / top, 0.0)
        root = lax.rsqrt(top)
        root = root * (1.5 - 0.5 * top * root * root)
        scaled = jnp.where(row == step, right * root, scaled)
        left = left - ratio * left[step : step + 1]
        right = right - ratio * right[step : step + 1]
    inverse_ref[...] = scaled
    own = terms[0][...]
    for term in terms[1:]:
        own = own + term[...]
    rows = white_ref.shape[0]
    white = jnp.dot(scaled[:, :size], own, precision=HI, preferred_element_type=F32)
    geno_var = own[SQUARE : SQUARE + 1] - jnp.sum(white * white, axis=0, keepdims=True)
    white = jnp.concatenate([white, jnp.zeros((LANES - size, own.shape[1]), F32)], axis=0)
    white_ref[...] = white.T[:rows]
    var_ref[...] = jnp.broadcast_to(geno_var, (LANES, own.shape[1])).T[:rows]


def solve(place, half_rows, rest_rows, terms, live, rows):
    half = half_rows.shape[0]
    wide = jax.ShapeDtypeStruct((rows, LANES), F32)
    return pl.pallas_call(
        functools.partial(solve_kernel, live, half, len(terms)),
        out_shape=(jax.ShapeDtypeStruct((2 * half, LANES), F32), wide, wide),
        in_specs=[SMEM] + [VMEM] * (2 + len(terms)),
        out_specs=(VMEM,) * 3,
        scratch_shapes=[pltpu.VMEM((2 * half, LANES), F32)],
        compiler_params=pltpu.CompilerParams(vmem_limit_bytes=LIMIT),
        cost_estimate=cost(5 * 10**9, 2**16),
        name="solve",
    )(place, half_rows, rest_rows, *terms)


def finish_kernel(dof, count, *refs):
    place_ref, inverse_ref, white_ref, var_ref, half_ref, rest_ref = refs[:6]
    terms, out_ref, small = refs[6 : 6 + count], refs[-2], refs[-1]
    half = half_ref.shape[0]
    rows, tile = out_ref.shape
    core = place_ref[1]
    low = pl.multiple_of(pl.program_id(0) * tile, tile)
    small[pl.ds(pl.multiple_of(core * half, half), half), :] = half_ref[:, pl.ds(low, tile)]
    small[pl.ds(pl.multiple_of((1 - core) * half, half), half), :] = rest_ref[:, pl.ds(low, tile)]
    white = jnp.dot(inverse_ref[:, : 2 * half], small[...], precision=HI, preferred_element_type=F32)
    pheno_var = small[SQUARE : SQUARE + 1, :] - jnp.sum(white * white, axis=0, keepdims=True)
    fitted = jnp.dot(white_ref[:, : 2 * half], white, precision=HI, preferred_element_type=F32)
    cross = terms[0][0:rows, pl.ds(low, tile)]
    for term in terms[1:]:
        cross = cross + term[0:rows, pl.ds(low, tile)]
    cross = cross - fitted
    out_ref[...] = cross * dof * lax.rsqrt(var_ref[:, 0:1] * pheno_var - cross * cross)


def finish(done, total, place, start, dof, inverse, white, geno_var, half_rows, rest_rows, terms):
    rows, width = terms[0].shape
    tile = min(TILE, width)
    first = start // tile
    args = [place, inverse, white, geno_var, half_rows, rest_rows, *terms]
    specs = [SMEM] + [VMEM] * (len(args) - 1)
    aliases = {}
    if done is not None:
        aliases = {len(args): 0}
        args.append(done)
        specs.append(HBM)
    return pl.pallas_call(
        functools.partial(finish_kernel, dof, len(terms)),
        grid=(width // tile,),
        out_shape=jax.ShapeDtypeStruct((rows, total), F32),
        in_specs=specs,
        out_specs=pl.BlockSpec((rows, tile), lambda j: (0, first + j)),
        scratch_shapes=[pltpu.VMEM((2 * half_rows.shape[0], tile), F32)],
        input_output_aliases=aliases,
        compiler_params=pltpu.CompilerParams(vmem_limit_bytes=LIMIT),
        cost_estimate=pl.CostEstimate(
            flops=2 * 256 * 256 * width, bytes_accessed=16 * rows * width, transcendentals=rows * width
        ),
    )(*args)


def fit_kernel(count, *refs):
    place_ref, inverse_ref, white_ref, half_ref, rest_ref = refs[:5]
    terms, (cross_ref, var_ref, small) = refs[5 : 5 + count], refs[5 + count :]
    half = half_ref.shape[0]
    core = place_ref[1]
    small[pl.ds(pl.multiple_of(core * half, half), half), :] = half_ref[...]
    small[pl.ds(pl.multiple_of((1 - core) * half, half), half), :] = rest_ref[...]
    white = jnp.dot(inverse_ref[:, : 2 * half], small[...], precision=HI, preferred_element_type=F32)
    pheno_var = small[SQUARE : SQUARE + 1, :] - jnp.sum(white * white, axis=0, keepdims=True)
    var_ref[...] = jnp.broadcast_to(pheno_var, var_ref.shape)
    fitted = jnp.dot(white_ref[:, : 2 * half], white, precision=HI, preferred_element_type=F32)
    cross = terms[0][...]
    for term in terms[1:]:
        cross = cross + term[...]
    cross_ref[...] = cross - fitted


def fit(place, inverse, white, half_rows, rest_rows, terms):
    rows, width = terms[0].shape
    args = [place, inverse, white, half_rows, rest_rows, *terms]
    return pl.pallas_call(
        functools.partial(fit_kernel, len(terms)),
        out_shape=(jax.ShapeDtypeStruct((rows, width), F32), jax.ShapeDtypeStruct((8, width), F32)),
        in_specs=[SMEM] + [VMEM] * (len(args) - 1),
        out_specs=(VMEM, VMEM),
        scratch_shapes=[pltpu.VMEM((2 * half_rows.shape[0], width), F32)],
        compiler_params=pltpu.CompilerParams(vmem_limit_bytes=LIMIT),
        cost_estimate=cost(2 * 256 * 256 * width, 16 * rows * width),
        name="fit",
    )(*args)


def close_kernel(dof, count, *refs):
    geno_var_ref, pheno_var_ref = refs[:2]
    terms, out_ref = refs[2 : 2 + count], refs[-1]
    tile = out_ref.shape[1]
    low = pl.multiple_of(pl.program_id(0) * tile, tile)
    cross = terms[0][:, pl.ds(low, tile)]
    for term in terms[1:]:
        cross = cross + term[:, pl.ds(low, tile)]
    pheno_var = pheno_var_ref[0:1, pl.ds(low, tile)]
    out_ref[...] = cross * dof * lax.rsqrt(geno_var_ref[:, 0:1] * pheno_var - cross * cross)


def close(done, total, start, dof, geno_var, pheno_var, terms):
    rows, width = terms[0].shape
    tile = min(TILE, width)
    first = start // tile
    args = [geno_var, pheno_var, *terms]
    specs = [VMEM] * len(args)
    aliases = {}
    if done is not None:
        aliases = {len(args): 0}
        args.append(done)
        specs.append(HBM)
    return pl.pallas_call(
        functools.partial(close_kernel, dof, len(terms)),
        grid=(width // tile,),
        out_shape=jax.ShapeDtypeStruct((rows, total), F32),
        in_specs=specs,
        out_specs=pl.BlockSpec((rows, tile), lambda j: (0, first + j)),
        input_output_aliases=aliases,
        compiler_params=pltpu.CompilerParams(vmem_limit_bytes=LIMIT),
        cost_estimate=cost(8 * rows * width, 12 * rows * width),
        name="close",
    )(*args)


def chunk_widths(total):
    units = total // TILE
    if total % TILE or units < 2:
        return [total]
    wide, odd = divmod(max(units - 4, 0), 2)
    sizes = [1] * min(units - units // 2, 2) + [2] * wide + [1] * odd + [1] * min(units // 2, 2)
    return [size * TILE for size in sizes]


def associate(dosage, phenotype, covariates):
    devices = lax.axis_size("subj")
    chips = devices // 2
    subjects, snps = dosage.shape
    verts = phenotype.shape[1]
    covs = covariates.shape[1]
    rows = snps // devices
    half = round_up(8 + covs, 16) // 2
    live = [0] + list(range(8, 8 + covs))
    place_index = lax.axis_index("subj")
    place = jnp.stack([place_index // 2, lax.rem(place_index, 2)]).astype(jnp.int32)
    sibling = [(i, i ^ 1) for i in range(devices)]

    def far_got(give_far):
        return lax.ppermute(give_far, "subj", sibling)

    def near_sums(parts, apart=False, got_far=None, unit=rows):
        far = (chips - 1) * unit
        give_far, give_near, keep_far, keep_near = parts
        if got_far is None:
            got_far = far_got(give_far)
        got_near = lax.ppermute(give_near, "subj", sibling)
        terms = [keep_near, got_near]
        if apart:
            blocks = [keep_far[low : low + unit] + got_far[low : low + unit] for low in range(0, far, unit)]
            return terms, blocks, keep_far[far:] + got_far[far:]
        summed = keep_far + got_far
        if chips == 2:
            return terms, [summed], summed[unit:]
        own_half = summed[far:]
        blocks = [jnp.concatenate([summed[low : low + unit], own_half], axis=0) for low in range(0, far, unit)]
        return terms, blocks, own_half

    def far_terms(blocks):
        came = []
        for step, block in enumerate(blocks, 1):
            moves = [(i, (i + 2 * step) % devices) for i in range(devices)]
            came.append(lax.ppermute(block, "subj", moves))
        return came

    def gather_half(halves, came):
        for block in came:
            halves = halves + block
        rest = lax.ppermute(halves, "subj", sibling)
        return halves, rest

    widths = chunk_widths(verts)
    last = len(widths)
    early = widths[:EARLY]
    left, geno, give_far, keep_far, *heres = open_up(place, dosage, covariates.T, phenotype, chips, rows, half, early)
    fars = [(give_far, keep_far, far_got(give_far))]
    for index in range(1, len(early)):
        give_far, keep_far = far_product(place, left, heres[index], chips, rows, half)
        fars.append((give_far, keep_far, far_got(give_far)))
    near, *nears = open_near(place, geno, heres, phenotype, widths[EARLY : EARLY + 1], rows)
    ahead = nears[2 * len(early) :]
    sums, came = [], []
    for index, (give_far, keep_far, got_far) in enumerate(fars):
        give_near, keep_near = nears[2 * index : 2 * index + 2]
        sums.append(near_sums((give_far, give_near, keep_far, keep_near), got_far=got_far))
        came.append(far_terms(sums[-1][1]))
    parts = with_design(place, left, geno, chips, rows, half)
    terms, blocks, own_half = near_sums(parts, unit=2 * half)
    base_came = far_terms(blocks)
    halves, rest = gather_half(own_half, [block[2 * half :] for block in base_came])
    inverse, white, geno_var = solve(
        place, halves, rest, terms + [block[: 2 * half] for block in base_came], live, rows
    )
    dof = float(subjects * devices - covs - 2) ** 0.5

    start = sum(early)
    for index in range(EARLY, last):
        tag = index + 1
        parts = product(place, left, near, ahead[0], phenotype, start, widths[index + 1 : index + 2], chips, rows, half)
        ahead = parts[4:]
        start += widths[index]
        sums.append(near_sums(parts[:4], apart=tag == last))
        if tag == last:
            last_half = far_terms([sums[-1][2]] * (chips - 1))
        came.append(far_terms(sums[-1][1]))
    out = None
    start = 0
    for index, width in enumerate(widths):
        tag = index + 1
        terms, _, own_half = sums[index]
        if tag < last:
            half_came = [block[rows:] for block in came[index]]
            halves, rest = gather_half(own_half, half_came)
            out = finish(
                out, verts, place, start, dof, inverse, white, geno_var, halves, rest, terms + came[index]
            )
        else:
            halves, rest = gather_half(own_half, last_half)
            cross, pheno_var = fit(place, inverse, white, halves, rest, terms)
            out = close(out, verts, start, dof, geno_var, pheno_var, [cross] + came[index])
        start += width
    return out


def solution(mesh):
    in_specs = (P(("grp", "subj"), None), P(("grp", "subj"), "vert"), P(("grp", "subj"), None))
    out_specs = P(("grp", "subj"), "vert")
    return jax.shard_map(associate, mesh=mesh, in_specs=in_specs, out_specs=out_specs, check_vma=False)
```
